256 devices in a mesh: section: 16 (over z, core), board: 16 (over y, x).
Axes of the slice: x: 4, y: 4, z: 8, core: 2. Of those that a mesh axis runs over, the one named last changes fastest.
Arguments:
- root_reach: float32 [2, 8, 1326], replicated, may hold values from 0.05 to 1
- frontier_value: float32 [2, 8, 1326], replicated, may hold values from -60 to 60
- regret_stop: float32 [16, 64, 8, 1326], P('section', 'board'), may hold values from 1 to 30
- regret_go: float32 [16, 64, 8, 1326], P('section', 'board'), may hold values from 1 to 30
- board_live: int32 [64], P('board'), may hold values from 0 to 1, as said below
- board_cards: int32 [64, 5], P('board'), may hold values from 0 to 51, as said below
- hand_rank: int32 [64, 1326], P('board'), may hold values from 0 to 1325
Outputs:
- new_stop: float32 [16, 64, 8, 1326], P('section', 'board')
- new_go: float32 [16, 64, 8, 1326], P('section', 'board')
- section_values: float32 [16, 2, 8, 1326], P('section')
The draws below stay inside these ranges and needn't reach their ends.
Inputs may be any that keep to these rules, and one draw needn't show every extreme that they name: `board_live`: 0 or 1; among each device's 4 slots the first one is always 1. `board_cards`: a slot's 5 cards are distinct. `hand_rank`: equal values tie.
All inputs are finite; a program needn't handle non-finite values.
Results may differ from the reference program's by a relative error of at most 0.0008.
Values sent between devices are 32-bit elements; how exact they have to be, the bound alone decides.
No kernel may reach another device: no remote copies, remote signals or barrier semaphores. Data moves between devices by JAX's collectives and lax.ppermute only.
A program may use at most 64 MiB of HBM per device.

```python
import math
import jax
import jax.numpy as jnp
import numpy as np
from jax import lax

CARDS = 52
BOARD_CARDS = 5
H = 1326
NODES = 8
BOARD_DEV = 4
SLOTS = 64
SECTIONS = 16


def draw_board_cards(key, part):
    keys = jax.random.split(jax.random.fold_in(key, 17), SLOTS)

    def one_board(board_key):
        return jax.random.permutation(board_key, CARDS)[:BOARD_CARDS].astype(jnp.int32)
    return jax.vmap(one_board)(keys)


def draw_board_live(key, part):
    coins = jax.random.randint(jax.random.fold_in(key, 29), (SLOTS,), 0, 2).astype(jnp.int32)
    leading = jnp.arange(SLOTS) % BOARD_DEV == 0
    return jnp.where(leading, 1, coins).astype(jnp.int32)


def place_ends(drawn, key, low, top_value):
    index_at = [jax.random.randint(jax.random.fold_in(key, axis), (), 0, length) for axis, length in enumerate(drawn.shape)]
    main_axis = drawn.shape.index(max(drawn.shape))
    next_to = index_at[:main_axis] + [(index_at[main_axis] + 1) % drawn.shape[main_axis]] + index_at[main_axis + 1:]
    return drawn.at[tuple(index_at)].set(low).at[tuple(next_to)].set(top_value)


def level_of(own_key, dims, shards, low, largest):
    loudness = 1.0
    for position, shards_of in shards:
        steps = jax.random.uniform(jax.random.fold_in(jax.random.fold_in(own_key, 6), position), (shards_of,), jnp.float32, low / len(shards), largest / len(shards))
        loudness = loudness * jnp.repeat(jnp.exp(steps), dims[position] // shards_of).reshape((-1,) + (1,) * (len(dims) - 1 - position))
    return loudness


def scatter_about(stream_key, dims, width, most, kind=jnp.bfloat16):
    values = jax.random.normal(stream_key, dims, jnp.float32) * width
    return jnp.minimum(jnp.maximum(values, -most), most).astype(kind)


def setup_inputs(seed: int = 0) -> dict:
    seeds = jax.random.split(jax.random.key(seed), 8)
    return {
        "root_reach": jnp.clip(jnp.exp(jax.random.uniform(seeds[0], (2, NODES, H), jnp.float32, math.log(0.05), math.log(1.0))), 0.05, 1.0),
        "frontier_value": scatter_about(seeds[1], (2, NODES, H), 10.0, 60.0, jnp.float32),
        "regret_stop": jnp.clip(jnp.exp(math.log(30.0) - 3.4011974 * jax.random.uniform(seeds[2], (SECTIONS, SLOTS, NODES, H), jnp.float32) ** level_of(seeds[2], (SECTIONS, SLOTS, NODES, H), ((0, 16), (1, 16)), -0.2, 0.2)), 1.0, 30.0),
        "regret_go": jnp.clip(jnp.exp(math.log(30.0) - 3.4011974 * jax.random.uniform(seeds[3], (SECTIONS, SLOTS, NODES, H), jnp.float32) ** level_of(seeds[3], (SECTIONS, SLOTS, NODES, H), ((0, 16), (1, 16)), -0.2, 0.2)), 1.0, 30.0),
        "board_live": draw_board_live(jax.random.fold_in(seeds[7], 71), 0),
        "board_cards": draw_board_cards(jax.random.fold_in(seeds[7], 71), 0),
        "hand_rank": place_ends(jax.random.randint(seeds[6], (SLOTS, H), 0, H), jax.random.fold_in(seeds[6], 1), 0, H - 1).astype(jnp.int32),
    }


def free_pairs():
    first, second = np.triu_indices(CARDS, 1)
    first = jnp.asarray(first.astype(np.int32))
    second = jnp.asarray(second.astype(np.int32))
    shared = (first[:, None] == first[None, :]) | (first[:, None] == second[None, :]) | (second[:, None] == first[None, :]) | (second[:, None] == second[None, :])
    return jnp.where(shared, 0.0, 1.0).astype(jnp.bfloat16)


def board_masks(board_cards):
    first, second = np.triu_indices(CARDS, 1)
    first = jnp.asarray(first.astype(np.int32))
    second = jnp.asarray(second.astype(np.int32))
    hits = (board_cards[:, :, None] == first[None, None, :]) | (board_cards[:, :, None] == second[None, None, :])
    return jnp.where(jnp.any(hits, axis=1), 0.0, 1.0).astype(jnp.float32)


def showdown(reach_one, stop_weight, mask_row, rank_row, disjoint):
    leaf_reach = (reach_one * stop_weight).astype(jnp.bfloat16)
    mask_half = mask_row.astype(jnp.bfloat16)
    payoff = jnp.sign(rank_row[:, None] - rank_row[None, :]).astype(jnp.bfloat16) * disjoint * mask_half[:, None] * mask_half[None, :]
    flipped = leaf_reach[::-1].reshape(-1, leaf_reach.shape[-1])
    result = jnp.dot(flipped.astype(jnp.float32), payoff.astype(jnp.float32).T, precision=lax.Precision.HIGHEST)
    return result.reshape(leaf_reach.shape)


def reference(root_reach, frontier_value, regret_stop, regret_go, board_live, board_cards, hand_rank):
    disjoint = free_pairs()
    masks = board_masks(board_cards)
    regret_sum = regret_stop + regret_go
    stop_prob = regret_stop / regret_sum
    go_prob = regret_go / regret_sum
    alive = (board_live > 0).astype(jnp.float32)
    board_total = jnp.sum(alive)
    depth_total = regret_stop.shape[0]
    players = jnp.arange(2)[:, None, None]
    reach_now = root_reach[None] * masks[:, None, None, :]
    leaf_store = []
    for level in range(depth_total):
        acting = players == level % 2
        factor = jnp.where(acting[None], go_prob[level][:, None], 1.0)
        stop_weight = jnp.where(acting[None], stop_prob[level][:, None], 1.0)

        def one_board(items):
            reach_one, weight_one, mask_row, rank_row, alive_one = items
            return lax.cond(alive_one > 0,
                            lambda: showdown(reach_one, weight_one, mask_row, rank_row, disjoint),
                            lambda: jnp.zeros(reach_one.shape, jnp.float32))

        leaf_values = lax.map(one_board, (reach_now, stop_weight, masks, hand_rank, alive))
        leaf_store.append(leaf_values)
        reach_now = reach_now * factor
    value_next = frontier_value[None] * masks[:, None, None, :]
    nexts = [None] * depth_total
    totals = [None] * depth_total
    for level in reversed(range(depth_total)):
        acting = players == level % 2
        factor = jnp.where(acting[None], go_prob[level][:, None], 1.0)
        stop_weight = jnp.where(acting[None], stop_prob[level][:, None], 1.0)
        nexts[level] = value_next
        value_next = stop_weight * leaf_store[level] + factor * value_next
        totals[level] = jnp.sum(alive[:, None, None, None] * value_next, axis=0) / board_total
    stops = []
    goes = []
    for level in range(depth_total):
        acting = players == level % 2
        own_next = jnp.sum(jnp.where(acting[None], nexts[level], 0.0), axis=1)
        own_leaf = jnp.sum(jnp.where(acting[None], leaf_store[level], 0.0), axis=1)
        gap = own_leaf - own_next
        keep_slot = alive[:, None, None] > 0
        stops.append(jnp.where(keep_slot, jnp.maximum(regret_stop[level] + go_prob[level] * gap, 0.0), regret_stop[level]))
        goes.append(jnp.where(keep_slot, jnp.maximum(regret_go[level] - stop_prob[level] * gap, 0.0), regret_go[level]))
    return (jnp.stack(stops), jnp.stack(goes), jnp.stack(totals))
```

```python
import jax
import jax.numpy as jnp
import numpy as np
from jax import lax
from jax.experimental import pallas as pl
from jax.experimental.pallas import tpu as pltpu
from jax.sharding import Mesh
from jax.sharding import PartitionSpec as P

CARDS = 52
H = 1326
W = 1408
NODES = 8
SLOTS = 4
DEPTHS = 16
PAIR = 2

VMEM = pl.BlockSpec(memory_space=pltpu.VMEM)
SMEM = pl.BlockSpec(memory_space=pltpu.SMEM)


def card_rows():
    first, second = np.triu_indices(CARDS, 1)
    rows = np.full((2, W), -1.0, np.float32)
    rows[0, :H] = first
    rows[1, :H] = second
    return jnp.asarray(rows)


def pack_go(stop_ref, go_ref, out_ref):
    out_ref[:, :, 1280:] = jnp.zeros((DEPTHS, PAIR, W - 1280), jnp.float32)
    for slot in range(SLOTS):
        go = go_ref[slot]
        prob = go / (stop_ref[slot] + go)
        for node in range(NODES):
            out_ref[slot // PAIR * NODES + node, slot % PAIR, :H] = prob[node]


def build_payoff(rank_ref, card_ref, out_ref):
    pair = lax.axis_index("section") // NODES
    rank = [rank_ref[pl.ds(PAIR * pair + i, 1), :].astype(jnp.float32) for i in range(PAIR)]
    first, second = card_ref[0:1, :], card_ref[1:2, :]
    rank = [jnp.concatenate([r, jnp.zeros((1, W - H), jnp.float32)], axis=1) for r in rank]
    rows = jnp.concatenate(rank + [first, second, jnp.zeros((4, W), jnp.float32)], axis=0)
    columns = rows.T
    step = 16
    for at in range(0, W, step):
        mine = columns[at : at + step]
        first_mine, second_mine = mine[:, 2:3], mine[:, 3:4]
        shared = (
            (first_mine == first)
            | (first_mine == second)
            | (second_mine == first)
            | (second_mine == second)
        )
        for i in range(PAIR):
            sign = jnp.clip(rank[i] - mine[:, i : i + 1], -1.0, 1.0)
            out_ref[i, at : at + step, :] = jnp.where(shared, 0.0, sign).astype(jnp.bfloat16)


def play(go_ref, payoff_ref, root_ref, frontier_ref, card_ref, board_ref, live_ref, out_ref, x_ref, leaf_ref, pad_ref):
    section = lax.axis_index("section")
    pair, node = section // NODES, section % NODES
    first, second = card_ref[0:1, :], card_ref[1:2, :]
    lane = lax.broadcasted_iota(jnp.int32, (1, W), 1)
    masks, alive = [], []
    for i in range(PAIR):
        free = lane < H
        for c in range(5):
            card = board_ref[PAIR * pair + i, c].astype(jnp.float32)
            free = free & (first != card) & (second != card)
        masks.append(jnp.where(free, 1.0, 0.0))
        alive.append((live_ref[PAIR * pair + i] > 0).astype(jnp.float32))
    mask = jnp.concatenate(masks, axis=0)
    pad_ref[:, 1280:] = jnp.zeros((4, W - 1280), jnp.float32)
    for p in range(2):
        pad_ref[p : p + 1, :H] = root_ref[p, pl.ds(node, 1), :]
        pad_ref[2 + p : 3 + p, :H] = frontier_ref[p, pl.ds(node, 1), :]
    reach = [pad_ref[p : p + 1, :] * mask for p in range(2)]
    for s in range(DEPTHS):
        q = s % 2
        go = go_ref[s]
        mine = reach[q] * (1.0 - go)
        for i in range(PAIR):
            x_ref[i, 2 * s + 1 - q, :] = mine[i]
            x_ref[i, 2 * s + q, :] = reach[1 - q][i]
        reach[q] = reach[q] * go
    for i in range(PAIR):
        leaf = jnp.dot(
            x_ref[i].astype(jnp.bfloat16), payoff_ref[i], preferred_element_type=jnp.float32
        )
        leaf_ref[:, i, :] = leaf * masks[i]
    value = [pad_ref[2 + p : 3 + p, :] * mask for p in range(2)]
    for s in reversed(range(DEPTHS)):
        q = s % 2
        go = go_ref[s]
        leaf_mine, leaf_other = leaf_ref[2 * s + q], leaf_ref[2 * s + 1 - q]
        out_ref[s, 0:PAIR, :] = leaf_mine - value[q]
        value[q] = (1.0 - go) * leaf_mine + go * value[q]
        value[1 - q] = leaf_other + value[1 - q]
        for p in range(2):
            total = alive[0] * value[p][0:1] + alive[1] * value[p][1:2]
            out_ref[s, PAIR + p : PAIR + p + 1, :] = total


def add_pairs(back_ref, live_ref, out_ref):
    live = jnp.float32(0.0)
    for slot in range(SLOTS):
        live += (live_ref[slot] > 0).astype(jnp.float32)
    lane = lax.broadcasted_iota(jnp.int32, (1, W), 1)
    for p in range(2):
        for node in range(NODES):
            at = PAIR + p
            total = back_ref[node, at : at + 1, :] + back_ref[NODES + node, at : at + 1, :]
            out_ref[p * NODES + node : p * NODES + node + 1, :] = jnp.where(lane == H, live, total)


def update(stop_ref, go_ref, back_ref, live_ref, new_stop_ref, new_go_ref, gap_ref):
    for slot in range(SLOTS):
        for node in range(NODES):
            gap_ref[slot, node, :] = back_ref[slot // PAIR * NODES + node, slot % PAIR, :]
    for slot in range(SLOTS):
        stop, go = stop_ref[slot], go_ref[slot]
        total = stop + go
        gap = gap_ref[slot, :, :H]
        keep = live_ref[slot] > 0
        new_stop_ref[slot] = jnp.where(keep, jnp.maximum(stop + go / total * gap, 0.0), stop)
        new_go_ref[slot] = jnp.where(keep, jnp.maximum(go - stop / total * gap, 0.0), go)


def call(body, out, specs, scratch=(), flops=100_000, limit=16 << 20):
    many = isinstance(out, list)
    return pl.pallas_call(
        body,
        out_shape=out,
        in_specs=specs,
        out_specs=[VMEM] * len(out) if many else VMEM,
        scratch_shapes=list(scratch),
        compiler_params=pltpu.CompilerParams(vmem_limit_bytes=limit),
        cost_estimate=pl.CostEstimate(flops=flops, bytes_accessed=400_000, transcendentals=0),
        name=body.__name__,
    )


def f32(*shape):
    return jax.ShapeDtypeStruct(shape, jnp.float32)


def add_over(value, axis):
    parts = [
        lax.ppermute(value, axis, [(k, (k + d) % 4) for k in range(4)]) for d in (2, 1, 3)
    ]
    return value + parts[0] + parts[1] + parts[2]


def local(root_reach, frontier_value, regret_stop, regret_go, board_live, board_cards, hand_rank):
    cards = card_rows()
    stop_now, go_now = regret_stop[0], regret_go[0]
    sent = call(pack_go, f32(DEPTHS, PAIR, W), [VMEM] * 2)(stop_now, go_now)
    go_all = lax.all_to_all(sent, "section", 0, 0, tiled=True)
    payoff = call(
        build_payoff,
        jax.ShapeDtypeStruct((PAIR, W, W), jnp.bfloat16),
        [VMEM] * 2,
        flops=20_000_000,
    )(hand_rank, cards)
    back = call(
        play,
        f32(DEPTHS, 2 * PAIR, W),
        [VMEM] * 5 + [SMEM] * 2,
        [
            pltpu.VMEM((PAIR, 2 * DEPTHS, W), jnp.float32),
            pltpu.VMEM((2 * DEPTHS, PAIR, W), jnp.float32),
            pltpu.VMEM((4, W), jnp.float32),
        ],
        flops=250_000_000,
        limit=24 << 20,
    )(go_all, payoff, root_reach, frontier_value, cards, board_cards, board_live)
    back = lax.all_to_all(back, "section", 0, 0, tiled=True)
    total = call(add_pairs, f32(2 * NODES, W), [VMEM, SMEM])(back, board_live)
    total = add_over(total, "x")
    total = add_over(total, "y")
    new_stop, new_go = call(
        update,
        [f32(SLOTS, NODES, H)] * 2,
        [VMEM] * 3 + [SMEM],
        [pltpu.VMEM((SLOTS, NODES, W), jnp.float32)],
        flops=2_000_000,
    )(stop_now, go_now, back, board_live)
    section_value = (total[:, :H] / total[:, H : H + 1]).reshape(1, 2, NODES, H)
    return (new_stop[None], new_go[None], section_value)


def solution(mesh):
    finer = Mesh(mesh.devices.reshape(16, 4, 4), ("section", "y", "x"))
    board = ("y", "x")
    return jax.shard_map(
        local,
        mesh=finer,
        in_specs=(
            P(),
            P(),
            P("section", board, None, None),
            P("section", board, None, None),
            P(board),
            P(board, None),
            P(board, None),
        ),
        out_specs=(
            P("section", board, None, None),
            P("section", board, None, None),
            P("section", None, None, None),
        ),
        check_vma=False,
    )
```

```python
import jax
import jax.numpy as jnp
import numpy as np
from jax import lax
from jax.experimental import pallas as pl
from jax.experimental.pallas import tpu as pltpu
from jax.sharding import Mesh
from jax.sharding import PartitionSpec as P

CARDS = 52
H = 1326
W = 1408
NODES = 8
SLOTS = 4
DEPTHS = 16
PAIR = 2
SIDE = 4
MOST = 60_000_000
CHUNKS = 4
CHUNK = W // CHUNKS

VMEM = pl.BlockSpec(memory_space=pltpu.VMEM)
SMEM = pl.BlockSpec(memory_space=pltpu.SMEM)
HBM = pl.BlockSpec(memory_space=pltpu.HBM)


def card_rows():
    first, second = np.triu_indices(CARDS, 1)
    rows = np.full((2, W), -1.0, np.float32)
    rows[0, :H] = first
    rows[1, :H] = second
    return jnp.asarray(rows)


def pack_go(stop_hbm, go_hbm, out_ref, stop_ref, go_ref, sem):
    copies = []
    for slot in range(SLOTS):
        for k, (src, dst) in enumerate(((stop_hbm, stop_ref), (go_hbm, go_ref))):
            copy = pltpu.make_async_copy(src.at[slot], dst.at[slot], sem.at[slot, k])
            copy.start()
            copies.append(copy)
    out_ref[:, :, 1280:] = jnp.zeros((DEPTHS, PAIR, W - 1280), jnp.float32)
    for slot in range(SLOTS):
        copies[2 * slot].wait()
        copies[2 * slot + 1].wait()
        go = go_ref[slot]
        prob = go / (stop_ref[slot] + go)
        for node in range(NODES):
            out_ref[slot // PAIR * NODES + node, slot % PAIR, :H] = prob[node]


def build_payoff(rank_ref, card_ref, out_hbm, out_ref, sem):
    pair = lax.axis_index("section") // NODES
    rank = [rank_ref[pl.ds(PAIR * pair + i, 1), :].astype(jnp.float32) for i in range(PAIR)]
    first, second = card_ref[0:1, :], card_ref[1:2, :]
    rank = [jnp.concatenate([r, jnp.zeros((1, W - H), jnp.float32)], axis=1) for r in rank]
    rows = jnp.concatenate(rank + [first, second, jnp.zeros((4, W), jnp.float32)], axis=0)
    columns = rows.T
    step = 16
    copies = []
    for at in range(0, W, step):
        mine = columns[at : at + step]
        first_mine, second_mine = mine[:, 2:3], mine[:, 3:4]
        shared = (
            (first_mine == first)
            | (first_mine == second)
            | (second_mine == first)
            | (second_mine == second)
        )
        for i in range(PAIR):
            sign = jnp.clip(rank[i] - mine[:, i : i + 1], -1.0, 1.0)
            out_ref[i, at : at + step, :] = jnp.where(shared, 0.0, sign).astype(jnp.bfloat16)
        if (at + step) % CHUNK == 0:
            for i in range(PAIR):
                rows_done = pl.ds(at + step - CHUNK, CHUNK)
                copy = pltpu.make_async_copy(
                    out_ref.at[i, rows_done], out_hbm.at[i, rows_done], sem.at[i, at // CHUNK]
                )
                copy.start()
                copies.append(copy)
    for copy in copies:
        copy.wait()


def play(
    go_ref, payoff_hbm, root_ref, frontier_ref, card_ref, board_ref, live_ref,
    sum_ref, gap_ref, payoff_ref, x_ref, leaf_ref, pad_ref, sem,
):
    copies = []
    for i in range(PAIR):
        for c in range(CHUNKS):
            rows = pl.ds(c * CHUNK, CHUNK)
            copy = pltpu.make_async_copy(
                payoff_hbm.at[i, rows], payoff_ref.at[i, rows], sem.at[i, c]
            )
            copy.start()
            copies.append(copy)
    section = lax.axis_index("section")
    pair, node = section // NODES, section % NODES
    first, second = card_ref[0:1, :], card_ref[1:2, :]
    lane = lax.broadcasted_iota(jnp.int32, (1, W), 1)
    masks, alive = [], []
    for i in range(PAIR):
        free = lane < H
        for c in range(5):
            card = board_ref[PAIR * pair + i, c].astype(jnp.float32)
            free = free & (first != card) & (second != card)
        masks.append(jnp.where(free, 1.0, 0.0))
        alive.append((live_ref[PAIR * pair + i] > 0).astype(jnp.float32))
    mask = jnp.concatenate(masks, axis=0)
    pad_ref[:, 1280:] = jnp.zeros((4, W - 1280), jnp.float32)
    for p in range(2):
        pad_ref[p : p + 1, :H] = root_ref[p, pl.ds(node, 1), :]
        pad_ref[2 + p : 3 + p, :H] = frontier_ref[p, pl.ds(node, 1), :]
    reach = [pad_ref[p : p + 1, :] * mask for p in range(2)]
    for s in range(DEPTHS):
        q = s % 2
        go = go_ref[s]
        mine = reach[q] * (1.0 - go)
        for i in range(PAIR):
            x_ref[i, 2 * s + 1 - q, :] = mine[i]
            x_ref[i, 2 * s + q, :] = reach[1 - q][i]
        reach[q] = reach[q] * go
    for i in range(PAIR):
        leaf = jnp.zeros((2 * DEPTHS, W), jnp.float32)
        for c in range(CHUNKS):
            copies[i * CHUNKS + c].wait()
            rows = slice(c * CHUNK, (c + 1) * CHUNK)
            leaf += jnp.dot(
                x_ref[i, :, rows].astype(jnp.bfloat16),
                payoff_ref[i, rows, :],
                preferred_element_type=jnp.float32,
            )
        leaf_ref[:, i, :] = leaf * masks[i]
    value = [pad_ref[2 + p : 3 + p, :] * mask for p in range(2)]
    for s in reversed(range(DEPTHS)):
        q = s % 2
        go = go_ref[s]
        leaf_mine, leaf_other = leaf_ref[2 * s + q], leaf_ref[2 * s + 1 - q]
        gap_ref[s] = leaf_mine - value[q]
        value[q] = (1.0 - go) * leaf_mine + go * value[q]
        value[1 - q] = leaf_other + value[1 - q]
        for p in range(2):
            total = alive[0] * value[p][0:1] + alive[1] * value[p][1:2]
            total = jnp.where(lane == H, alive[0] + alive[1], total)
            sum_ref[s, p : p + 1, :] = total


def add_pairs(part_ref, out_ref):
    for p in range(2):
        for node in range(NODES):
            total = part_ref[node, p : p + 1, :] + part_ref[NODES + node, p : p + 1, :]
            out_ref[p * NODES + node : p * NODES + node + 1, :] = total


def finish(own_ref, *refs):
    out_ref = refs[-1]
    total = own_ref[...]
    for part_ref in refs[:-1]:
        total += part_ref[...]
    value = total[:, :H] / total[:, H : H + 1]
    for p in range(2):
        out_ref[p] = value[p * NODES : (p + 1) * NODES]


def update(stop_ref, go_ref, back_ref, live_ref, new_stop_ref, new_go_ref, gap_ref):
    for slot in range(SLOTS):
        for node in range(NODES):
            gap_ref[slot, node, :] = back_ref[slot // PAIR * NODES + node, slot % PAIR, :]
    for slot in range(SLOTS):
        stop, go = stop_ref[slot], go_ref[slot]
        total = stop + go
        gap = gap_ref[slot, :, :H]
        keep = live_ref[slot] > 0
        new_stop_ref[slot] = jnp.where(keep, jnp.maximum(stop + go / total * gap, 0.0), stop)
        new_go_ref[slot] = jnp.where(keep, jnp.maximum(go - stop / total * gap, 0.0), go)


def call(body, out, specs, scratch=(), flops=100_000, limit=16 << 20, out_spec=VMEM):
    many = isinstance(out, list)
    return pl.pallas_call(
        body,
        out_shape=out,
        in_specs=specs,
        out_specs=[out_spec] * len(out) if many else out_spec,
        scratch_shapes=list(scratch),
        compiler_params=pltpu.CompilerParams(vmem_limit_bytes=limit),
        cost_estimate=pl.CostEstimate(flops=flops, bytes_accessed=400_000, transcendentals=0),
        name=body.__name__,
    )


def f32(*shape):
    return jax.ShapeDtypeStruct(shape, jnp.float32)


def from_others(value, axis):
    return [
        lax.ppermute(value, axis, [(k, (k + d) % SIDE) for k in range(SIDE)]) for d in (2, 1, 3)
    ]


def local(root_reach, frontier_value, regret_stop, regret_go, board_live, board_cards, hand_rank):
    cards = card_rows()
    stop_now, go_now = regret_stop[0], regret_go[0]
    block = pltpu.VMEM((SLOTS, NODES, H), jnp.float32)
    sent = call(
        pack_go,
        f32(DEPTHS, PAIR, W),
        [HBM] * 2,
        [block, block, pltpu.SemaphoreType.DMA((SLOTS, 2))],
        limit=67_000_000,
    )(stop_now, go_now)
    go_all = lax.all_to_all(sent, "section", 0, 0, tiled=True)
    payoff = call(
        build_payoff,
        jax.ShapeDtypeStruct((PAIR, W, W), jnp.bfloat16),
        [VMEM] * 2,
        [pltpu.VMEM((PAIR, W, W), jnp.bfloat16), pltpu.SemaphoreType.DMA((PAIR, CHUNKS))],
        flops=20_000_000,
        limit=MOST,
        out_spec=HBM,
    )(hand_rank, cards)
    sums, gaps = call(
        play,
        [f32(DEPTHS, 2, W), f32(DEPTHS, PAIR, W)],
        [VMEM, HBM] + [VMEM] * 3 + [SMEM] * 2,
        [
            pltpu.VMEM((PAIR, W, W), jnp.bfloat16),
            pltpu.VMEM((PAIR, 2 * DEPTHS, W), jnp.float32),
            pltpu.VMEM((2 * DEPTHS, PAIR, W), jnp.float32),
            pltpu.VMEM((4, W), jnp.float32),
            pltpu.SemaphoreType.DMA((PAIR, CHUNKS)),
        ],
        flops=250_000_000,
        limit=MOST,
    )(go_all, payoff, root_reach, frontier_value, cards, board_cards, board_live)
    sums = lax.all_to_all(sums, "section", 0, 0, tiled=True)
    gaps = lax.all_to_all(gaps, "section", 0, 0, tiled=True)
    total = call(add_pairs, f32(2 * NODES, W), [VMEM])(sums)
    total = sum(from_others(total, "x"), start=total)
    parts = from_others(total, "y")
    new_stop, new_go = call(
        update,
        [f32(SLOTS, NODES, H)] * 2,
        [VMEM] * 3 + [SMEM],
        [pltpu.VMEM((SLOTS, NODES, W), jnp.float32)],
        flops=2_000_000,
    )(stop_now, go_now, gaps, board_live)
    section_value = call(finish, f32(2, NODES, H), [VMEM] * SIDE)(total, *parts)
    return (new_stop[None], new_go[None], section_value[None])


def solution(mesh):
    finer = Mesh(mesh.devices.reshape(DEPTHS, SIDE, SIDE), ("section", "y", "x"))
    board = ("y", "x")
    return jax.shard_map(
        local,
        mesh=finer,
        in_specs=(
            P(),
            P(),
            P("section", board, None, None),
            P("section", board, None, None),
            P(board),
            P(board, None),
            P(board, None),
        ),
        out_specs=(
            P("section", board, None, None),
            P("section", board, None, None),
            P("section", None, None, None),
        ),
        check_vma=False,
    )
```

```python
import jax
import jax.numpy as jnp
import numpy as np
from jax import lax
from jax.experimental import pallas as pl
from jax.experimental.pallas import tpu as pltpu
from jax.sharding import Mesh
from jax.sharding import PartitionSpec as P

CARDS = 52
H = 1326
W = 1408
NODES = 8
SLOTS = 4
DEPTHS = 16
PAIR = 2
SIDE = 4
MOST = 60_000_000
PAYOFF = jnp.float4_e2m1fn

VMEM = pl.BlockSpec(memory_space=pltpu.VMEM)
SMEM = pl.BlockSpec(memory_space=pltpu.SMEM)
HBM = pl.BlockSpec(memory_space=pltpu.HBM)


def card_masks():
    hands = np.zeros((2, W), np.uint32)
    for cards in np.triu_indices(CARDS, 1):
        for word in range(2):
            inside = cards // 32 == word
            hands[word, :H] |= np.where(inside, np.uint32(1) << (cards % 32).astype(np.uint32), 0).astype(np.uint32)
    return jnp.asarray(hands.view(np.int32))


def pack_go(stop_hbm, go_hbm, rank_hbm, card_hbm, out_ref, rank_out, card_out, stop_ref, go_ref, rank_ref, sem):
    copies = []
    for slot in range(SLOTS):
        for k, (src, dst) in enumerate(((stop_hbm, stop_ref), (go_hbm, go_ref))):
            copy = pltpu.make_async_copy(src.at[slot], dst.at[slot], sem.at[slot, k])
            copy.start()
            copies.append(copy)
    rank_copy = pltpu.make_async_copy(rank_hbm, rank_ref, sem.at[SLOTS, 0])
    card_copy = pltpu.make_async_copy(card_hbm, card_out, sem.at[SLOTS, 1])
    rank_copy.start()
    card_copy.start()
    out_ref[:, :, 1280:] = jnp.zeros((DEPTHS, PAIR, W - 1280), jnp.float32)
    rank_out[...] = jnp.zeros((8, W), jnp.float32)
    for slot in range(SLOTS):
        copies[2 * slot].wait()
        copies[2 * slot + 1].wait()
        go = go_ref[slot]
        prob = go / (stop_ref[slot] + go)
        for node in range(NODES):
            out_ref[slot // PAIR * NODES + node, slot % PAIR, :H] = prob[node]
    rank_copy.wait()
    pair = lax.axis_index("section") // NODES
    for i in range(PAIR):
        rank_out[i : i + 1, :H] = rank_ref[pl.ds(PAIR * pair + i, 1), :].astype(jnp.float32)
    card_copy.wait()


def build_payoff(rank_ref, card_ref, out_ref):
    rank_column = rank_ref[...].T
    low, high = card_ref[0:1, :], card_ref[1:2, :]
    card_column = jnp.concatenate([card_ref[...], jnp.zeros((6, W), jnp.int32)], axis=0).T
    step = 64
    for at in range(0, W, step):
        mine = rank_column[at : at + step]
        low_mine = card_column[at : at + step, 0:1]
        high_mine = card_column[at : at + step, 1:2]
        free = ((low_mine & low) | (high_mine & high)) == 0
        for i in range(PAIR):
            sign = jnp.clip(rank_ref[i : i + 1, :] - mine[:, i : i + 1], -1.0, 1.0)
            out_ref[i, at : at + step, :] = jnp.where(free, sign, 0.0).astype(PAYOFF)


def play(
    go_ref, payoff_ref, root_ref, frontier_ref, card_ref, board_ref, live_ref,
    sum_ref, gap_ref, x_ref, leaf_ref, pad_ref,
):
    section = lax.axis_index("section")
    pair, node = section // NODES, section % NODES
    low, high = card_ref[0:1, :], card_ref[1:2, :]
    lane = lax.broadcasted_iota(jnp.int32, (1, W), 1)
    masks, alive = [], []
    for i in range(PAIR):
        words = [jnp.int32(0), jnp.int32(0)]
        for c in range(5):
            card = board_ref[PAIR * pair + i, c]
            bit = lax.shift_left(jnp.int32(1), card & 31)
            words[0] |= jnp.where(card < 32, bit, 0)
            words[1] |= jnp.where(card < 32, 0, bit)
        free = (((low & words[0]) | (high & words[1])) == 0) & (lane < H)
        masks.append(jnp.where(free, 1.0, 0.0))
        alive.append((live_ref[PAIR * pair + i] > 0).astype(jnp.float32))
    mask = jnp.concatenate(masks, axis=0)
    pad_ref[:, 1280:] = jnp.zeros((4, W - 1280), jnp.float32)
    for p in range(2):
        pad_ref[p : p + 1, :H] = root_ref[p, pl.ds(node, 1), :]
        pad_ref[2 + p : 3 + p, :H] = frontier_ref[p, pl.ds(node, 1), :]
    reach = [pad_ref[p : p + 1, :] * mask for p in range(2)]
    for s in range(DEPTHS):
        q = s % 2
        go = go_ref[s]
        mine = reach[q] * (1.0 - go)
        for i in range(PAIR):
            x_ref[i, 2 * s + 1 - q, :] = mine[i]
            x_ref[i, 2 * s + q, :] = reach[1 - q][i]
        reach[q] = reach[q] * go
    for i in range(PAIR):
        leaf = jnp.dot(
            x_ref[i].astype(jnp.bfloat16),
            payoff_ref[i].astype(jnp.bfloat16),
            preferred_element_type=jnp.float32,
        )
        leaf_ref[:, i, :] = leaf * masks[i]
    value = [pad_ref[2 + p : 3 + p, :] * mask for p in range(2)]
    for s in reversed(range(DEPTHS)):
        q = s % 2
        go = go_ref[s]
        leaf_mine, leaf_other = leaf_ref[2 * s + q], leaf_ref[2 * s + 1 - q]
        gap_ref[s] = leaf_mine - value[q]
        value[q] = (1.0 - go) * leaf_mine + go * value[q]
        value[1 - q] = leaf_other + value[1 - q]
        for p in range(2):
            total = alive[0] * value[p][0:1] + alive[1] * value[p][1:2]
            total = jnp.where(lane == H, alive[0] + alive[1], total)
            sum_ref[s, p : p + 1, :] = total


def add_pairs(part_ref, out_ref):
    for p in range(2):
        for node in range(NODES):
            total = part_ref[node, p : p + 1, :] + part_ref[NODES + node, p : p + 1, :]
            out_ref[p * NODES + node : p * NODES + node + 1, :] = total


def finish(own_ref, *refs):
    out_ref = refs[-1]
    total = own_ref[...]
    for part_ref in refs[:-1]:
        total += part_ref[...]
    value = total[:, :H] / total[:, H : H + 1]
    for p in range(2):
        out_ref[p] = value[p * NODES : (p + 1) * NODES]


def update(stop_ref, go_ref, back_ref, live_ref, after_ref, new_stop_hbm, new_go_hbm, new_stop_ref, new_go_ref, gap_ref, sem):
    copies = []
    for slot in range(SLOTS):
        for node in range(NODES):
            gap_ref[node, :] = back_ref[slot // PAIR * NODES + node, slot % PAIR, :]
        stop, go = stop_ref[slot], go_ref[slot]
        total = stop + go
        gap = gap_ref[:, :H]
        keep = live_ref[slot] > 0
        new_stop_ref[slot] = jnp.where(keep, jnp.maximum(stop + go / total * gap, 0.0), stop)
        new_go_ref[slot] = jnp.where(keep, jnp.maximum(go - stop / total * gap, 0.0), go)
        for k, (src, dst) in enumerate(((new_stop_ref, new_stop_hbm), (new_go_ref, new_go_hbm))):
            copy = pltpu.make_async_copy(src.at[slot], dst.at[slot], sem.at[slot, k])
            copy.start()
            copies.append(copy)
    for copy in copies:
        copy.wait()


def call(body, out, specs, scratch=(), flops=100_000, limit=24 << 20, out_spec=VMEM):
    many = isinstance(out, list)
    return pl.pallas_call(
        body,
        out_shape=out,
        in_specs=specs,
        out_specs=[out_spec] * len(out) if many else out_spec,
        scratch_shapes=list(scratch),
        compiler_params=pltpu.CompilerParams(vmem_limit_bytes=limit),
        cost_estimate=pl.CostEstimate(flops=flops, bytes_accessed=400_000, transcendentals=0),
        name=body.__name__,
    )


def in_hbm(value):
    return pltpu.with_memory_space_constraint(value, pltpu.HBM)


def f32(*shape):
    return jax.ShapeDtypeStruct(shape, jnp.float32)


def from_others(value, axis):
    return [
        lax.ppermute(value, axis, [(k, k ^ d) for k in range(SIDE)]) for d in (3, 1, 2)
    ]


def local(root_reach, frontier_value, regret_stop, regret_go, board_live, board_cards, hand_rank):
    stop_now, go_now = regret_stop[0], regret_go[0]
    block = pltpu.VMEM((SLOTS, NODES, H), jnp.float32)
    sent, ranks, cards = call(
        pack_go,
        [
            pltpu.VMEM((DEPTHS, PAIR, W), jnp.float32),
            pltpu.VMEM((8, W), jnp.float32),
            pltpu.VMEM((2, W), jnp.int32),
        ],
        [HBM] * 4,
        [
            block,
            block,
            pltpu.VMEM((SLOTS, H), jnp.int32),
            pltpu.SemaphoreType.DMA((SLOTS + 1, 2)),
        ],
    )(*[in_hbm(a) for a in (stop_now, go_now, hand_rank, card_masks())])
    go_all = lax.all_to_all(sent, "section", 0, 0, tiled=True)
    payoff = call(
        build_payoff,
        jax.ShapeDtypeStruct((PAIR, W, W), PAYOFF),
        [VMEM] * 2,
        flops=20_000_000,
    )(ranks, cards)
    sums, gaps = call(
        play,
        [pltpu.VMEM((DEPTHS, 2, W), jnp.float32), f32(DEPTHS, PAIR, W)],
        [VMEM] * 5 + [SMEM] * 2,
        [
            pltpu.VMEM((PAIR, 2 * DEPTHS, W), jnp.float32),
            pltpu.VMEM((2 * DEPTHS, PAIR, W), jnp.float32),
            pltpu.VMEM((4, W), jnp.float32),
        ],
        flops=250_000_000,
    )(go_all, payoff, root_reach, frontier_value, cards, board_cards, board_live)
    sums = lax.all_to_all(sums, "section", 0, 0, tiled=True)
    gaps = lax.all_to_all(gaps, "section", 0, 0, tiled=True)
    total = call(add_pairs, f32(2 * NODES, W), [VMEM])(sums)
    total = sum(from_others(total, "x"), start=total)
    parts = from_others(total, "y")
    section_value = call(finish, f32(2, NODES, H), [VMEM] * SIDE)(total, *parts)
    new_stop, new_go = call(
        update,
        [f32(SLOTS, NODES, H)] * 2,
        [VMEM] * 3 + [SMEM, HBM],
        [block, block, pltpu.VMEM((NODES, W), jnp.float32), pltpu.SemaphoreType.DMA((SLOTS, 2))],
        flops=2_000_000,
        out_spec=HBM,
    )(stop_now, go_now, gaps, board_live, in_hbm(section_value))
    return (new_stop[None], new_go[None], section_value[None])


def solution(mesh):
    finer = Mesh(mesh.devices.reshape(DEPTHS, SIDE, SIDE), ("section", "y", "x"))
    board = ("y", "x")
    return jax.shard_map(
        local,
        mesh=finer,
        in_specs=(
            P(),
            P(),
            P("section", board, None, None),
            P("section", board, None, None),
            P(board),
            P(board, None),
            P(board, None),
        ),
        out_specs=(
            P("section", board, None, None),
            P("section", board, None, None),
            P("section", None, None, None),
        ),
        check_vma=False,
    )
```

```python
import jax
import jax.numpy as jnp
import numpy as np
from jax import lax
from jax.experimental import pallas as pl
from jax.experimental.pallas import tpu as pltpu
from jax.sharding import Mesh
from jax.sharding import PartitionSpec as P

CARDS = 52
H = 1326
W = 1408
NODES = 8
SLOTS = 4
DEPTHS = 16
PAIR = 2
SIDE = 4
MOST = 60_000_000
PAYOFF = jnp.float4_e2m1fn

VMEM = pl.BlockSpec(memory_space=pltpu.VMEM)
HBM = pl.BlockSpec(memory_space=pltpu.HBM)


def card_masks():
    hands = np.zeros((2, W), np.uint32)
    for cards in np.triu_indices(CARDS, 1):
        for word in range(2):
            inside = cards // 32 == word
            hands[word, :H] |= np.where(inside, np.uint32(1) << (cards % 32).astype(np.uint32), 0).astype(np.uint32)
    return jnp.asarray(hands.view(np.int32))


def pack_go(stop_hbm, go_hbm, rank_hbm, card_hbm, out_ref, rank_out, card_out, stop_ref, go_ref, rank_ref, sem):
    copies = []
    for slot in range(SLOTS):
        for k, (src, dst) in enumerate(((stop_hbm, stop_ref), (go_hbm, go_ref))):
            copy = pltpu.make_async_copy(src.at[slot], dst.at[slot], sem.at[slot, k])
            copy.start()
            copies.append(copy)
    rank_copy = pltpu.make_async_copy(rank_hbm, rank_ref, sem.at[SLOTS, 0])
    card_copy = pltpu.make_async_copy(card_hbm, card_out, sem.at[SLOTS, 1])
    rank_copy.start()
    card_copy.start()
    out_ref[:, :, 1280:] = jnp.ones((DEPTHS, PAIR, W - 1280), jnp.float32)
    rank_out[...] = jnp.zeros((8, W), jnp.float32)
    for slot in range(SLOTS):
        copies[2 * slot].wait()
        copies[2 * slot + 1].wait()
        go = go_ref[slot]
        prob = go / (stop_ref[slot] + go)
        for node in range(NODES):
            out_ref[slot // PAIR * NODES + node, slot % PAIR, :H] = prob[node]
    rank_copy.wait()
    pair = lax.axis_index("section") // NODES
    for i in range(PAIR):
        rank_out[i : i + 1, :H] = rank_ref[pl.ds(PAIR * pair + i, 1), :].astype(jnp.float32)
    card_copy.wait()


def prepare(
    rank_ref, card_ref, root_hbm, frontier_hbm, board_hbm, live_hbm,
    payoff_ref, reach_ref, value_ref, mask_ref, alive_ref, pair_ref,
    root_ref, frontier_ref, board_ref, live_ref, sem,
):
    copies = [
        pltpu.make_async_copy(src, dst, sem.at[k])
        for k, (src, dst) in enumerate(
            (
                (root_hbm, root_ref),
                (frontier_hbm, frontier_ref),
                (board_hbm, board_ref),
                (live_hbm, live_ref),
            )
        )
    ]
    for copy in copies:
        copy.start()
    low, high = card_ref[0:1, :], card_ref[1:2, :]
    rank_column = rank_ref[...].T
    card_column = jnp.concatenate([card_ref[...], jnp.zeros((6, W), jnp.int32)], axis=0).T
    step = 64
    for at in range(0, W, step):
        mine = rank_column[at : at + step]
        low_mine = card_column[at : at + step, 0:1]
        high_mine = card_column[at : at + step, 1:2]
        free = ((low_mine & low) | (high_mine & high)) == 0
        for i in range(PAIR):
            sign = jnp.clip(rank_ref[i : i + 1, :] - mine[:, i : i + 1], -1.0, 1.0)
            payoff_ref[i, at : at + step, :] = jnp.where(free, sign, 0.0).astype(PAYOFF)
    for copy in copies:
        copy.wait()
    section = lax.axis_index("section")
    pair, node = section // NODES, section % NODES
    lane = lax.broadcasted_iota(jnp.int32, (1, W), 1)
    for slot in range(SLOTS):
        alive_ref[slot : slot + 1, :] = jnp.broadcast_to(
            (live_ref[slot] > 0).astype(jnp.float32), (1, W)
        )
    for i in range(PAIR):
        words = [jnp.int32(0), jnp.int32(0)]
        for c in range(5):
            card = board_ref[PAIR * pair + i, c]
            bit = lax.shift_left(jnp.int32(1), card & 31)
            words[0] |= jnp.where(card < 32, bit, 0)
            words[1] |= jnp.where(card < 32, 0, bit)
        free = (((low & words[0]) | (high & words[1])) == 0) & (lane < H)
        mask_ref[i : i + 1, :] = jnp.where(free, 1.0, 0.0)
        pair_ref[i : i + 1, :] = jnp.broadcast_to(
            (live_ref[PAIR * pair + i] > 0).astype(jnp.float32), (1, W)
        )
    mask = mask_ref[...]
    for p in range(2):
        reach_ref[p] = jnp.zeros((PAIR, W), jnp.float32)
        value_ref[p] = jnp.where(lane == H, 1.0, jnp.zeros((PAIR, W), jnp.float32))
        reach_ref[p, :, :H] = root_ref[p, pl.ds(node, 1), :] * mask[:, :H]
        value_ref[p, :, :H] = frontier_ref[p, pl.ds(node, 1), :] * mask[:, :H]


def play(
    go_ref, payoff_ref, reach_ref, value_ref, mask_ref, alive_ref, sum_ref, gap_ref, x_ref, leaf_ref
):
    reach = [reach_ref[p] for p in range(2)]
    for s in range(DEPTHS):
        q = s % 2
        go = go_ref[s]
        mine = reach[q] * (1.0 - go)
        for i in range(PAIR):
            x_ref[i, 2 * s + 1 - q, :] = mine[i]
            x_ref[i, 2 * s + q, :] = reach[1 - q][i]
        reach[q] = reach[q] * go
    for i in range(PAIR):
        leaf = jnp.dot(
            x_ref[i].astype(jnp.bfloat16),
            payoff_ref[i].astype(jnp.bfloat16),
            preferred_element_type=jnp.float32,
        )
        leaf_ref[:, i, :] = leaf * mask_ref[i : i + 1, :]
    value = [value_ref[p] for p in range(2)]
    alive = alive_ref[...]
    for s in reversed(range(DEPTHS)):
        q = s % 2
        go = go_ref[s]
        leaf_mine, leaf_other = leaf_ref[2 * s + q], leaf_ref[2 * s + 1 - q]
        gap_ref[s] = leaf_mine - value[q]
        value[q] = (1.0 - go) * leaf_mine + go * value[q]
        value[1 - q] = leaf_other + value[1 - q]
        for p in range(2):
            weighted = alive * value[p]
            sum_ref[s, p : p + 1, :] = weighted[0:1] + weighted[1:2]


def add_pairs(part_ref, out_ref):
    for p in range(2):
        for node in range(NODES):
            total = part_ref[node, p : p + 1, :] + part_ref[NODES + node, p : p + 1, :]
            out_ref[p * NODES + node : p * NODES + node + 1, :] = total


def conclude(
    own_ref, part_x, part_y, part_z, stop_ref, go_ref, back_ref, alive_ref,
    new_stop_hbm, new_go_hbm, value_hbm,
    new_stop_ref, new_go_ref, value_ref, gap_ref, sem,
):
    total = own_ref[...] + part_x[...] + part_y[...] + part_z[...]
    value = total[:, :H] / total[:, H : H + 1]
    for p in range(2):
        value_ref[p] = value[p * NODES : (p + 1) * NODES]
    copies = [pltpu.make_async_copy(value_ref, value_hbm, sem.at[SLOTS, 0])]
    copies[0].start()
    for slot in range(SLOTS):
        for node in range(NODES):
            gap_ref[slot, node, :] = back_ref[slot // PAIR * NODES + node, slot % PAIR, :]
        stop, go = stop_ref[slot], go_ref[slot]
        total = stop + go
        gap = gap_ref[slot, :, :H]
        keep = alive_ref[slot : slot + 1, :H] > 0
        new_stop_ref[slot] = jnp.where(keep, jnp.maximum(stop + go / total * gap, 0.0), stop)
        new_go_ref[slot] = jnp.where(keep, jnp.maximum(go - stop / total * gap, 0.0), go)
        for k, (src, dst) in enumerate(((new_stop_ref, new_stop_hbm), (new_go_ref, new_go_hbm))):
            copy = pltpu.make_async_copy(src.at[slot], dst.at[slot], sem.at[slot, k])
            copy.start()
            copies.append(copy)
    for copy in copies:
        copy.wait()


def call(body, out, specs, scratch=(), flops=100_000, limit=24 << 20, out_spec=VMEM):
    many = isinstance(out, list)
    return pl.pallas_call(
        body,
        out_shape=out,
        in_specs=specs,
        out_specs=[out_spec] * len(out) if many else out_spec,
        scratch_shapes=list(scratch),
        compiler_params=pltpu.CompilerParams(vmem_limit_bytes=limit),
        cost_estimate=pl.CostEstimate(flops=flops, bytes_accessed=400_000, transcendentals=0),
        name=body.__name__,
    )


def in_hbm(value):
    return pltpu.with_memory_space_constraint(value, pltpu.HBM)


def f32(*shape):
    return jax.ShapeDtypeStruct(shape, jnp.float32)


def from_others(value, axis):
    return [
        lax.ppermute(value, axis, [(k, k ^ d) for k in range(SIDE)]) for d in (3, 1, 2)
    ]


def local(root_reach, frontier_value, regret_stop, regret_go, board_live, board_cards, hand_rank):
    stop_now, go_now = regret_stop[0], regret_go[0]
    block = pltpu.VMEM((SLOTS, NODES, H), jnp.float32)
    sent, ranks, cards = call(
        pack_go,
        [
            pltpu.VMEM((DEPTHS, PAIR, W), jnp.float32),
            pltpu.VMEM((8, W), jnp.float32),
            pltpu.VMEM((2, W), jnp.int32),
        ],
        [HBM] * 4,
        [
            block,
            block,
            pltpu.VMEM((SLOTS, H), jnp.int32),
            pltpu.SemaphoreType.DMA((SLOTS + 1, 2)),
        ],
    )(*[in_hbm(a) for a in (stop_now, go_now, hand_rank, card_masks())])
    go_all = lax.all_to_all(sent, "section", 0, 0, tiled=True)
    payoff, reach, value, mask, alive, alive_pair = call(
        prepare,
        [
            jax.ShapeDtypeStruct((PAIR, W, W), PAYOFF),
            f32(2, PAIR, W),
            f32(2, PAIR, W),
            f32(PAIR, W),
            f32(SLOTS, W),
            f32(PAIR, W),
        ],
        [VMEM] * 2 + [HBM] * 4,
        [
            pltpu.VMEM((2, NODES, H), jnp.float32),
            pltpu.VMEM((2, NODES, H), jnp.float32),
            pltpu.SMEM((SLOTS, 5), jnp.int32),
            pltpu.SMEM((SLOTS,), jnp.int32),
            pltpu.SemaphoreType.DMA((4,)),
        ],
        flops=20_000_000,
    )(ranks, cards, *[in_hbm(a) for a in (root_reach, frontier_value, board_cards, board_live)])
    sums, gaps = call(
        play,
        [pltpu.VMEM((DEPTHS, 2, W), jnp.float32), pltpu.VMEM((DEPTHS, PAIR, W), jnp.float32)],
        [VMEM] * 6,
        [
            pltpu.VMEM((PAIR, 2 * DEPTHS, W), jnp.float32),
            pltpu.VMEM((2 * DEPTHS, PAIR, W), jnp.float32),
        ],
        flops=250_000_000,
    )(go_all, payoff, reach, value, mask, alive_pair)
    sums = lax.all_to_all(sums, "section", 0, 0, tiled=True)
    gaps = lax.all_to_all(gaps, "section", 0, 0, tiled=True)
    total = call(add_pairs, f32(2 * NODES, W), [VMEM])(sums)
    total = sum(from_others(total, "x"), start=total)
    parts = from_others(total, "y")
    new_stop, new_go, section_value = call(
        conclude,
        [f32(SLOTS, NODES, H), f32(SLOTS, NODES, H), f32(2, NODES, H)],
        [VMEM] * 8,
        [
            block,
            block,
            pltpu.VMEM((2, NODES, H), jnp.float32),
            pltpu.VMEM((SLOTS, NODES, W), jnp.float32),
            pltpu.SemaphoreType.DMA((SLOTS + 1, 2)),
        ],
        flops=2_000_000,
        out_spec=HBM,
    )(total, *parts, stop_now, go_now, gaps, alive)
    return (new_stop[None], new_go[None], section_value[None])


def solution(mesh):
    finer = Mesh(mesh.devices.reshape(DEPTHS, SIDE, SIDE), ("section", "y", "x"))
    board = ("y", "x")
    return jax.shard_map(
        local,
        mesh=finer,
        in_specs=(
            P(),
            P(),
            P("section", board, None, None),
            P("section", board, None, None),
            P(board),
            P(board, None),
            P(board, None),
        ),
        out_specs=(
            P("section", board, None, None),
            P("section", board, None, None),
            P("section", None, None, None),
        ),
        check_vma=False,
    )
```

```python
import jax
import jax.numpy as jnp
import numpy as np
from jax import lax
from jax.experimental import pallas as pl
from jax.experimental.pallas import tpu as pltpu
from jax.sharding import Mesh
from jax.sharding import PartitionSpec as P

CARDS = 52
H = 1326
W = 1408
NODES = 8
SLOTS = 4
DEPTHS = 16
ORDER = [*range(15, -1, -2), *range(14, -1, -2)]
PLACE = [ORDER.index(s) for s in range(DEPTHS)]
PAIR = 2
SIDE = 4
MOST = 60_000_000
PAYOFF = jnp.float4_e2m1fn

VMEM = pl.BlockSpec(memory_space=pltpu.VMEM)
HBM = pl.BlockSpec(memory_space=pltpu.HBM)


def card_masks():
    hands = np.zeros((2, W), np.uint32)
    for cards in np.triu_indices(CARDS, 1):
        for word in range(2):
            inside = cards // 32 == word
            hands[word, :H] |= np.where(inside, np.uint32(1) << (cards % 32).astype(np.uint32), 0).astype(np.uint32)
    return jnp.asarray(hands.view(np.int32))


def pack_go(stop_hbm, go_hbm, rank_hbm, card_hbm, out_ref, rank_out, card_out, stop_ref, go_ref, rank_ref, sem):
    copies = []
    for slot in range(SLOTS):
        for k, (src, dst) in enumerate(((stop_hbm, stop_ref), (go_hbm, go_ref))):
            copy = pltpu.make_async_copy(src.at[slot], dst.at[slot], sem.at[slot, k])
            copy.start()
            copies.append(copy)
    rank_copy = pltpu.make_async_copy(rank_hbm, rank_ref, sem.at[SLOTS, 0])
    card_copy = pltpu.make_async_copy(card_hbm, card_out, sem.at[SLOTS, 1])
    rank_copy.start()
    card_copy.start()
    out_ref[:, :, 1280:] = jnp.ones((DEPTHS, PAIR, W - 1280), jnp.float32)
    rank_out[...] = jnp.zeros((8, W), jnp.float32)
    for slot in range(SLOTS):
        copies[2 * slot].wait()
        copies[2 * slot + 1].wait()
        go = go_ref[slot]
        prob = go / (stop_ref[slot] + go)
        for node in range(NODES):
            out_ref[PLACE[slot // PAIR * NODES + node], slot % PAIR, :H] = prob[node]
    rank_copy.wait()
    pair = lax.axis_index("section") // NODES
    for i in range(PAIR):
        rank_out[i : i + 1, :H] = rank_ref[pl.ds(PAIR * pair + i, 1), :].astype(jnp.float32)
    card_copy.wait()


def prepare(
    rank_ref, card_ref, root_hbm, frontier_hbm, board_hbm, live_hbm,
    payoff_ref, reach_ref, value_ref, mask_ref, alive_ref, pair_ref,
    root_ref, frontier_ref, board_ref, live_ref, sem,
):
    copies = [
        pltpu.make_async_copy(src, dst, sem.at[k])
        for k, (src, dst) in enumerate(
            (
                (root_hbm, root_ref),
                (frontier_hbm, frontier_ref),
                (board_hbm, board_ref),
                (live_hbm, live_ref),
            )
        )
    ]
    for copy in copies:
        copy.start()
    low, high = card_ref[0:1, :], card_ref[1:2, :]
    rank_column = rank_ref[...].T
    card_column = jnp.concatenate([card_ref[...], jnp.zeros((6, W), jnp.int32)], axis=0).T
    step = 64
    for at in range(0, W, step):
        mine = rank_column[at : at + step]
        low_mine = card_column[at : at + step, 0:1]
        high_mine = card_column[at : at + step, 1:2]
        free = ((low_mine & low) | (high_mine & high)) == 0
        for i in range(PAIR):
            sign = jnp.clip(rank_ref[i : i + 1, :] - mine[:, i : i + 1], -1.0, 1.0)
            payoff_ref[i, at : at + step, :] = jnp.where(free, sign, 0.0).astype(PAYOFF)
    for copy in copies:
        copy.wait()
    section = lax.axis_index("section")
    pair, node = section // NODES, section % NODES
    lane = lax.broadcasted_iota(jnp.int32, (1, W), 1)
    for slot in range(SLOTS):
        alive_ref[slot : slot + 1, :] = jnp.broadcast_to(
            (live_ref[slot] > 0).astype(jnp.float32), (1, W)
        )
    for i in range(PAIR):
        words = [jnp.int32(0), jnp.int32(0)]
        for c in range(5):
            card = board_ref[PAIR * pair + i, c]
            bit = lax.shift_left(jnp.int32(1), card & 31)
            words[0] |= jnp.where(card < 32, bit, 0)
            words[1] |= jnp.where(card < 32, 0, bit)
        free = (((low & words[0]) | (high & words[1])) == 0) & (lane < H)
        mask_ref[i : i + 1, :] = jnp.where(free, 1.0, 0.0)
        pair_ref[i : i + 1, :] = jnp.broadcast_to(
            (live_ref[PAIR * pair + i] > 0).astype(jnp.float32), (1, W)
        )
    mask = mask_ref[...]
    for p in range(2):
        reach_ref[p] = jnp.zeros((PAIR, W), jnp.float32)
        value_ref[p] = jnp.where(lane == H, 1.0, jnp.zeros((PAIR, W), jnp.float32))
        reach_ref[p, :, :H] = root_ref[p, pl.ds(node, 1), :] * mask[:, :H]
        value_ref[p, :, :H] = frontier_ref[p, pl.ds(node, 1), :] * mask[:, :H]


def play(
    go_ref, payoff_ref, reach_ref, value_ref, mask_ref, alive_ref, sum_ref, gap_ref, x_ref, leaf_ref
):
    reach = [reach_ref[p] for p in range(2)]
    for s in range(DEPTHS):
        q = s % 2
        go = go_ref[PLACE[s]]
        mine = reach[q] * (1.0 - go)
        for i in range(PAIR):
            x_ref[i, 2 * s + 1 - q, :] = mine[i]
            x_ref[i, 2 * s + q, :] = reach[1 - q][i]
        reach[q] = reach[q] * go
    for i in range(PAIR):
        leaf = jnp.dot(
            x_ref[i].astype(jnp.bfloat16),
            payoff_ref[i].astype(jnp.bfloat16),
            preferred_element_type=jnp.float32,
        )
        leaf_ref[:, i, :] = leaf * mask_ref[i : i + 1, :]
    value = [value_ref[p] for p in range(2)]
    alive = alive_ref[...]
    for s in reversed(range(DEPTHS)):
        q = s % 2
        go = go_ref[PLACE[s]]
        leaf_mine, leaf_other = leaf_ref[2 * s + q], leaf_ref[2 * s + 1 - q]
        gap_ref[PLACE[s]] = leaf_mine - value[q]
        value[q] = (1.0 - go) * leaf_mine + go * value[q]
        value[1 - q] = leaf_other + value[1 - q]
        for p in range(2):
            weighted = alive * value[p]
            sum_ref[PLACE[s], p : p + 1, :] = weighted[0:1] + weighted[1:2]


def add_pairs(part_ref, out_ref):
    for p in range(2):
        for node in range(NODES):
            pair = [part_ref[PLACE[i * NODES + node], p : p + 1, :] for i in range(2)]
            total = pair[0] + pair[1]
            out_ref[p * NODES + node : p * NODES + node + 1, :] = total


def conclude(
    own_ref, part_x, part_y, part_z, stop_ref, go_ref, back_ref, alive_ref,
    new_stop_hbm, new_go_hbm, value_hbm,
    new_stop_ref, new_go_ref, value_ref, gap_ref, sem,
):
    total = own_ref[...] + part_x[...] + part_y[...] + part_z[...]
    value = total[:, :H] / total[:, H : H + 1]
    for p in range(2):
        value_ref[p] = value[p * NODES : (p + 1) * NODES]
    copies = [pltpu.make_async_copy(value_ref, value_hbm, sem.at[SLOTS, 0])]
    copies[0].start()
    for slot in range(SLOTS):
        for node in range(NODES):
            gap_ref[slot, node, :] = back_ref[PLACE[slot // PAIR * NODES + node], slot % PAIR, :]
        stop, go = stop_ref[slot], go_ref[slot]
        total = stop + go
        gap = gap_ref[slot, :, :H]
        keep = alive_ref[slot : slot + 1, :H] > 0
        new_stop_ref[slot] = jnp.where(keep, jnp.maximum(stop + go / total * gap, 0.0), stop)
        new_go_ref[slot] = jnp.where(keep, jnp.maximum(go - stop / total * gap, 0.0), go)
        for k, (src, dst) in enumerate(((new_stop_ref, new_stop_hbm), (new_go_ref, new_go_hbm))):
            copy = pltpu.make_async_copy(src.at[slot], dst.at[slot], sem.at[slot, k])
            copy.start()
            copies.append(copy)
    for copy in copies:
        copy.wait()


def call(body, out, specs, scratch=(), flops=100_000, limit=24 << 20, out_spec=VMEM):
    many = isinstance(out, list)
    return pl.pallas_call(
        body,
        out_shape=out,
        in_specs=specs,
        out_specs=[out_spec] * len(out) if many else out_spec,
        scratch_shapes=list(scratch),
        compiler_params=pltpu.CompilerParams(vmem_limit_bytes=limit),
        cost_estimate=pl.CostEstimate(flops=flops, bytes_accessed=400_000, transcendentals=0),
        name=body.__name__,
    )


def in_hbm(value):
    return pltpu.with_memory_space_constraint(value, pltpu.HBM)


def f32(*shape):
    return jax.ShapeDtypeStruct(shape, jnp.float32)


def exchange(value):
    return lax.all_to_all(value, "section", 0, 0, axis_index_groups=[ORDER], tiled=True)


def from_others(value, axis):
    return [
        lax.ppermute(value, axis, [(k, k ^ d) for k in range(SIDE)]) for d in (3, 1, 2)
    ]


def local(root_reach, frontier_value, regret_stop, regret_go, board_live, board_cards, hand_rank):
    stop_now, go_now = regret_stop[0], regret_go[0]
    block = pltpu.VMEM((SLOTS, NODES, H), jnp.float32)
    sent, ranks, cards = call(
        pack_go,
        [
            pltpu.VMEM((DEPTHS, PAIR, W), jnp.float32),
            pltpu.VMEM((8, W), jnp.float32),
            pltpu.VMEM((2, W), jnp.int32),
        ],
        [HBM] * 4,
        [
            block,
            block,
            pltpu.VMEM((SLOTS, H), jnp.int32),
            pltpu.SemaphoreType.DMA((SLOTS + 1, 2)),
        ],
    )(*[in_hbm(a) for a in (stop_now, go_now, hand_rank, card_masks())])
    go_all = exchange(sent)
    payoff, reach, value, mask, alive, alive_pair = call(
        prepare,
        [
            jax.ShapeDtypeStruct((PAIR, W, W), PAYOFF),
            f32(2, PAIR, W),
            f32(2, PAIR, W),
            f32(PAIR, W),
            f32(SLOTS, W),
            f32(PAIR, W),
        ],
        [VMEM] * 2 + [HBM] * 4,
        [
            pltpu.VMEM((2, NODES, H), jnp.float32),
            pltpu.VMEM((2, NODES, H), jnp.float32),
            pltpu.SMEM((SLOTS, 5), jnp.int32),
            pltpu.SMEM((SLOTS,), jnp.int32),
            pltpu.SemaphoreType.DMA((4,)),
        ],
        flops=20_000_000,
    )(ranks, cards, *[in_hbm(a) for a in (root_reach, frontier_value, board_cards, board_live)])
    sums, gaps = call(
        play,
        [pltpu.VMEM((DEPTHS, 2, W), jnp.float32), pltpu.VMEM((DEPTHS, PAIR, W), jnp.float32)],
        [VMEM] * 6,
        [
            pltpu.VMEM((PAIR, 2 * DEPTHS, W), jnp.float32),
            pltpu.VMEM((2 * DEPTHS, PAIR, W), jnp.float32),
        ],
        flops=250_000_000,
    )(go_all, payoff, reach, value, mask, alive_pair)
    sums = exchange(sums)
    gaps = exchange(gaps)
    total = call(add_pairs, f32(2 * NODES, W), [VMEM])(sums)
    total = sum(from_others(total, "x"), start=total)
    parts = from_others(total, "y")
    new_stop, new_go, section_value = call(
        conclude,
        [f32(SLOTS, NODES, H), f32(SLOTS, NODES, H), f32(2, NODES, H)],
        [VMEM] * 8,
        [
            block,
            block,
            pltpu.VMEM((2, NODES, H), jnp.float32),
            pltpu.VMEM((SLOTS, NODES, W), jnp.float32),
            pltpu.SemaphoreType.DMA((SLOTS + 1, 2)),
        ],
        flops=2_000_000,
        out_spec=HBM,
    )(total, *parts, stop_now, go_now, gaps, alive)
    return (new_stop[None], new_go[None], section_value[None])


def solution(mesh):
    finer = Mesh(mesh.devices.reshape(DEPTHS, SIDE, SIDE), ("section", "y", "x"))
    board = ("y", "x")
    return jax.shard_map(
        local,
        mesh=finer,
        in_specs=(
            P(),
            P(),
            P("section", board, None, None),
            P("section", board, None, None),
            P(board),
            P(board, None),
            P(board, None),
        ),
        out_specs=(
            P("section", board, None, None),
            P("section", board, None, None),
            P("section", None, None, None),
        ),
        check_vma=False,
    )
```

```python
import jax
import jax.numpy as jnp
import numpy as np
from jax import lax
from jax.experimental import pallas as pl
from jax.experimental.pallas import tpu as pltpu
from jax.sharding import Mesh
from jax.sharding import PartitionSpec as P

CARDS = 52
H = 1326
W = 1408
NODES = 8
SLOTS = 4
DEPTHS = 16
ORDER = [*range(15, -1, -2), *range(14, -1, -2)]
PLACE = [ORDER.index(s) for s in range(DEPTHS)]
PAIR = 2
SIDE = 4
MOST = 60_000_000
PAYOFF = jnp.float4_e2m1fn

VMEM = pl.BlockSpec(memory_space=pltpu.VMEM)
HBM = pl.BlockSpec(memory_space=pltpu.HBM)


def card_masks():
    hands = np.zeros((2, W), np.uint32)
    for cards in np.triu_indices(CARDS, 1):
        for word in range(2):
            inside = cards // 32 == word
            hands[word, :H] |= np.where(inside, np.uint32(1) << (cards % 32).astype(np.uint32), 0).astype(np.uint32)
    return jnp.asarray(hands.view(np.int32))


def pack_go(stop_hbm, go_hbm, rank_hbm, card_hbm, out_ref, rank_out, card_out, stop_ref, go_ref, rank_ref, sem):
    copies = []
    for slot in range(SLOTS):
        for k, (src, dst) in enumerate(((stop_hbm, stop_ref), (go_hbm, go_ref))):
            copy = pltpu.make_async_copy(src.at[slot], dst.at[slot], sem.at[slot, k])
            copy.start()
            copies.append(copy)
    rank_copy = pltpu.make_async_copy(rank_hbm, rank_ref, sem.at[SLOTS, 0])
    card_copy = pltpu.make_async_copy(card_hbm, card_out, sem.at[SLOTS, 1])
    rank_copy.start()
    card_copy.start()
    out_ref[:, :, 1280:] = jnp.ones((DEPTHS, PAIR, W - 1280), jnp.float32)
    rank_out[...] = jnp.zeros((8, W), jnp.float32)
    for slot in range(SLOTS):
        copies[2 * slot].wait()
        copies[2 * slot + 1].wait()
        go = go_ref[slot]
        prob = go / (stop_ref[slot] + go)
        for node in range(NODES):
            out_ref[PLACE[slot // PAIR * NODES + node], slot % PAIR, :H] = prob[node]
    rank_copy.wait()
    pair = lax.axis_index("section") // NODES
    for i in range(PAIR):
        rank_out[i : i + 1, :H] = rank_ref[pl.ds(PAIR * pair + i, 1), :].astype(jnp.float32)
    card_copy.wait()


def prepare(
    rank_ref, card_ref, root_hbm, frontier_hbm, board_hbm, live_hbm,
    payoff_ref, reach_ref, value_ref, mask_ref, alive_ref, pair_ref,
    root_ref, frontier_ref, board_ref, live_ref, sem,
):
    copies = [
        pltpu.make_async_copy(src, dst, sem.at[k])
        for k, (src, dst) in enumerate(
            (
                (root_hbm, root_ref),
                (frontier_hbm, frontier_ref),
                (board_hbm, board_ref),
                (live_hbm, live_ref),
            )
        )
    ]
    for copy in copies:
        copy.start()
    low, high = card_ref[0:1, :], card_ref[1:2, :]
    rank_column = rank_ref[...].T
    card_column = jnp.concatenate([card_ref[...], jnp.zeros((6, W), jnp.int32)], axis=0).T
    step = 64
    for at in range(0, W, step):
        mine = rank_column[at : at + step]
        low_mine = card_column[at : at + step, 0:1]
        high_mine = card_column[at : at + step, 1:2]
        free = ((low_mine & low) | (high_mine & high)) == 0
        for i in range(PAIR):
            sign = jnp.clip(rank_ref[i : i + 1, :] - mine[:, i : i + 1], -1.0, 1.0)
            payoff_ref[i, at : at + step, :] = jnp.where(free, sign, 0.0).astype(PAYOFF)
    for copy in copies:
        copy.wait()
    section = lax.axis_index("section")
    pair, node = section // NODES, section % NODES
    lane = lax.broadcasted_iota(jnp.int32, (1, W), 1)
    for slot in range(SLOTS):
        alive_ref[slot : slot + 1, :] = jnp.broadcast_to(
            (live_ref[slot] > 0).astype(jnp.float32), (1, W)
        )
    for i in range(PAIR):
        words = [jnp.int32(0), jnp.int32(0)]
        for c in range(5):
            card = board_ref[PAIR * pair + i, c]
            bit = lax.shift_left(jnp.int32(1), card & 31)
            words[0] |= jnp.where(card < 32, bit, 0)
            words[1] |= jnp.where(card < 32, 0, bit)
        free = (((low & words[0]) | (high & words[1])) == 0) & (lane < H)
        mask_ref[i : i + 1, :] = jnp.where(free, 1.0, 0.0)
        pair_ref[i : i + 1, :] = jnp.broadcast_to(
            (live_ref[PAIR * pair + i] > 0).astype(jnp.float32), (1, W)
        )
    mask = mask_ref[...]
    for p in range(2):
        reach_ref[p] = jnp.zeros((PAIR, W), jnp.float32)
        value_ref[p] = jnp.where(lane == H, 1.0, jnp.zeros((PAIR, W), jnp.float32))
        reach_ref[p, :, :H] = root_ref[p, pl.ds(node, 1), :] * mask[:, :H]
        value_ref[p, :, :H] = frontier_ref[p, pl.ds(node, 1), :] * mask[:, :H]


def play(
    go_ref, payoff_ref, reach_ref, value_ref, mask_ref, alive_ref, sum_ref, gap_ref, x_ref, leaf_ref
):
    reach = [reach_ref[p] for p in range(2)]
    for s in range(DEPTHS):
        q = s % 2
        go = go_ref[PLACE[s]]
        mine = reach[q] * (1.0 - go)
        for i in range(PAIR):
            x_ref[i, 2 * s + 1 - q, :] = mine[i]
            x_ref[i, 2 * s + q, :] = reach[1 - q][i]
        reach[q] = reach[q] * go
    for i in range(PAIR):
        leaf = jnp.dot(
            x_ref[i].astype(jnp.bfloat16),
            payoff_ref[i].astype(jnp.bfloat16),
            preferred_element_type=jnp.float32,
        )
        leaf_ref[:, i, :] = leaf * mask_ref[i : i + 1, :]
    value = [value_ref[p] for p in range(2)]
    alive = alive_ref[...]
    for s in reversed(range(DEPTHS)):
        q = s % 2
        go = go_ref[PLACE[s]]
        leaf_mine, leaf_other = leaf_ref[2 * s + q], leaf_ref[2 * s + 1 - q]
        gap_ref[PLACE[s]] = leaf_mine - value[q]
        value[q] = (1.0 - go) * leaf_mine + go * value[q]
        value[1 - q] = leaf_other + value[1 - q]
        for p in range(2):
            weighted = alive * value[p]
            sum_ref[PLACE[s], p : p + 1, :] = weighted[0:1] + weighted[1:2]


def add_pairs(part_ref, out_ref):
    for p in range(2):
        for node in range(NODES):
            pair = [part_ref[PLACE[i * NODES + node], p : p + 1, :] for i in range(2)]
            total = pair[0] + pair[1]
            out_ref[p * NODES + node : p * NODES + node + 1, :] = total


def conclude(
    own_ref, part_x, part_y, part_z, stop_ref, go_ref, back_ref, alive_ref,
    new_stop_hbm, new_go_hbm, value_hbm,
    new_stop_ref, new_go_ref, value_ref, gap_ref, sem,
):
    total = own_ref[...] + part_x[...] + part_y[...] + part_z[...]
    value = total[:, :H] / total[:, H : H + 1]
    for p in range(2):
        value_ref[p] = value[p * NODES : (p + 1) * NODES]
    copies = [pltpu.make_async_copy(value_ref, value_hbm, sem.at[SLOTS, 0])]
    copies[0].start()
    for slot in range(SLOTS):
        for node in range(NODES):
            gap_ref[slot, node, :] = back_ref[PLACE[slot // PAIR * NODES + node], slot % PAIR, :]
        stop, go = stop_ref[slot], go_ref[slot]
        total = stop + go
        gap = gap_ref[slot, :, :H]
        keep = alive_ref[slot : slot + 1, :H] > 0
        new_stop_ref[slot] = jnp.where(keep, jnp.maximum(stop + go / total * gap, 0.0), stop)
        new_go_ref[slot] = jnp.where(keep, jnp.maximum(go - stop / total * gap, 0.0), go)
        for k, (src, dst) in enumerate(((new_stop_ref, new_stop_hbm), (new_go_ref, new_go_hbm))):
            copy = pltpu.make_async_copy(src.at[slot], dst.at[slot], sem.at[slot, k])
            copy.start()
            copies.append(copy)
    for copy in copies:
        copy.wait()


def call(body, out, specs, scratch=(), flops=100_000, limit=24 << 20, out_spec=VMEM):
    many = isinstance(out, list)
    return pl.pallas_call(
        body,
        out_shape=out,
        in_specs=specs,
        out_specs=[out_spec] * len(out) if many else out_spec,
        scratch_shapes=list(scratch),
        compiler_params=pltpu.CompilerParams(vmem_limit_bytes=limit),
        cost_estimate=pl.CostEstimate(flops=flops, bytes_accessed=400_000, transcendentals=0),
        name=body.__name__,
    )


def in_hbm(value):
    return pltpu.with_memory_space_constraint(value, pltpu.HBM)


def f32(*shape):
    return jax.ShapeDtypeStruct(shape, jnp.float32)


def exchange(value):
    return lax.all_to_all(value, "section", 0, 0, axis_index_groups=[ORDER], tiled=True)


def from_others(value, axis):
    return [
        lax.ppermute(value, axis, [(k, k ^ d) for k in range(SIDE)]) for d in (3, 1, 2)
    ]


def local(root_reach, frontier_value, regret_stop, regret_go, board_live, board_cards, hand_rank):
    stop_now, go_now = regret_stop[0], regret_go[0]
    block = pltpu.VMEM((SLOTS, NODES, H), jnp.float32)
    sent, ranks, cards = call(
        pack_go,
        [
            pltpu.VMEM((DEPTHS, PAIR, W), jnp.float32),
            pltpu.VMEM((8, W), jnp.float32),
            pltpu.VMEM((2, W), jnp.int32),
        ],
        [HBM] * 4,
        [
            block,
            block,
            pltpu.VMEM((SLOTS, H), jnp.int32),
            pltpu.SemaphoreType.DMA((SLOTS + 1, 2)),
        ],
    )(*[in_hbm(a) for a in (stop_now, go_now, hand_rank, card_masks())])
    go_all = exchange(sent)
    payoff, reach, value, mask, alive, alive_pair = call(
        prepare,
        [
            jax.ShapeDtypeStruct((PAIR, W, W), PAYOFF),
            f32(2, PAIR, W),
            f32(2, PAIR, W),
            f32(PAIR, W),
            f32(SLOTS, W),
            f32(PAIR, W),
        ],
        [VMEM] * 2 + [HBM] * 4,
        [
            pltpu.VMEM((2, NODES, H), jnp.float32),
            pltpu.VMEM((2, NODES, H), jnp.float32),
            pltpu.SMEM((SLOTS, 5), jnp.int32),
            pltpu.SMEM((SLOTS,), jnp.int32),
            pltpu.SemaphoreType.DMA((4,)),
        ],
        flops=20_000_000,
    )(ranks, cards, *[in_hbm(a) for a in (root_reach, frontier_value, board_cards, board_live)])
    sums, gaps = call(
        play,
        [pltpu.VMEM((DEPTHS, 2, W), jnp.float32), pltpu.VMEM((DEPTHS, PAIR, W), jnp.float32)],
        [VMEM] * 6,
        [
            pltpu.VMEM((PAIR, 2 * DEPTHS, W), jnp.float32),
            pltpu.VMEM((2 * DEPTHS, PAIR, W), jnp.float32),
        ],
        flops=250_000_000,
    )(go_all, payoff, reach, value, mask, alive_pair)
    sums = exchange(sums)
    gaps = exchange(gaps)
    total = call(add_pairs, f32(2 * NODES, W), [VMEM])(sums)
    total = sum(from_others(total, "y"), start=total)
    parts = from_others(total, "x")
    new_stop, new_go, section_value = call(
        conclude,
        [f32(SLOTS, NODES, H), f32(SLOTS, NODES, H), f32(2, NODES, H)],
        [VMEM] * 8,
        [
            block,
            block,
            pltpu.VMEM((2, NODES, H), jnp.float32),
            pltpu.VMEM((SLOTS, NODES, W), jnp.float32),
            pltpu.SemaphoreType.DMA((SLOTS + 1, 2)),
        ],
        flops=2_000_000,
        out_spec=HBM,
    )(total, *parts, stop_now, go_now, gaps, alive)
    return (new_stop[None], new_go[None], section_value[None])


def solution(mesh):
    finer = Mesh(mesh.devices.reshape(DEPTHS, SIDE, SIDE), ("section", "y", "x"))
    board = ("y", "x")
    return jax.shard_map(
        local,
        mesh=finer,
        in_specs=(
            P(),
            P(),
            P("section", board, None, None),
            P("section", board, None, None),
            P(board),
            P(board, None),
            P(board, None),
        ),
        out_specs=(
            P("section", board, None, None),
            P("section", board, None, None),
            P("section", None, None, None),
        ),
        check_vma=False,
    )
```

```python
import jax
import jax.numpy as jnp
import numpy as np
from jax import lax
from jax.experimental import pallas as pl
from jax.experimental.pallas import tpu as pltpu
from jax.sharding import Mesh
from jax.sharding import PartitionSpec as P

CARDS = 52
H = 1326
W = 1408
NODES = 8
SLOTS = 4
DEPTHS = 16
ORDER = [*range(15, -1, -2), *range(14, -1, -2)]
PLACE = [ORDER.index(s) for s in range(DEPTHS)]
SUM_ORDER = [*range(15, -1, -2), *range(0, 16, 2)]
SUM_PLACE = [SUM_ORDER.index(s) for s in range(DEPTHS)]
PAIR = 2
SIDE = 4
MOST = 60_000_000
PAYOFF = jnp.float4_e2m1fn

VMEM = pl.BlockSpec(memory_space=pltpu.VMEM)
HBM = pl.BlockSpec(memory_space=pltpu.HBM)


def card_masks():
    hands = np.zeros((2, W), np.uint32)
    for cards in np.triu_indices(CARDS, 1):
        for word in range(2):
            inside = cards // 32 == word
            hands[word, :H] |= np.where(inside, np.uint32(1) << (cards % 32).astype(np.uint32), 0).astype(np.uint32)
    return jnp.asarray(hands.view(np.int32))


def pack_go(stop_hbm, go_hbm, rank_hbm, card_hbm, out_ref, rank_out, card_out, stop_ref, go_ref, rank_ref, sem):
    copies = []
    for slot in range(SLOTS):
        for k, (src, dst) in enumerate(((stop_hbm, stop_ref), (go_hbm, go_ref))):
            copy = pltpu.make_async_copy(src.at[slot], dst.at[slot], sem.at[slot, k])
            copy.start()
            copies.append(copy)
    rank_copy = pltpu.make_async_copy(rank_hbm, rank_ref, sem.at[SLOTS, 0])
    card_copy = pltpu.make_async_copy(card_hbm, card_out, sem.at[SLOTS, 1])
    rank_copy.start()
    card_copy.start()
    out_ref[:, :, 1280:] = jnp.ones((DEPTHS, PAIR, W - 1280), jnp.float32)
    rank_out[...] = jnp.zeros((8, W), jnp.float32)
    for slot in range(SLOTS):
        copies[2 * slot].wait()
        copies[2 * slot + 1].wait()
        go = go_ref[slot]
        prob = go / (stop_ref[slot] + go)
        for node in range(NODES):
            out_ref[PLACE[slot // PAIR * NODES + node], slot % PAIR, :H] = prob[node]
    rank_copy.wait()
    pair = lax.axis_index("section") // NODES
    for i in range(PAIR):
        rank_out[i : i + 1, :H] = rank_ref[pl.ds(PAIR * pair + i, 1), :].astype(jnp.float32)
    card_copy.wait()


def prepare(
    rank_ref, card_ref, root_hbm, frontier_hbm, board_hbm, live_hbm,
    payoff_ref, reach_ref, value_ref, mask_ref, alive_ref, pair_ref,
    root_ref, frontier_ref, board_ref, live_ref, sem,
):
    copies = [
        pltpu.make_async_copy(src, dst, sem.at[k])
        for k, (src, dst) in enumerate(
            (
                (root_hbm, root_ref),
                (frontier_hbm, frontier_ref),
                (board_hbm, board_ref),
                (live_hbm, live_ref),
            )
        )
    ]
    for copy in copies:
        copy.start()
    low, high = card_ref[0:1, :], card_ref[1:2, :]
    rank_column = rank_ref[...].T
    card_column = jnp.concatenate([card_ref[...], jnp.zeros((6, W), jnp.int32)], axis=0).T
    step = 64
    for at in range(0, W, step):
        mine = rank_column[at : at + step]
        low_mine = card_column[at : at + step, 0:1]
        high_mine = card_column[at : at + step, 1:2]
        free = ((low_mine & low) | (high_mine & high)) == 0
        for i in range(PAIR):
            sign = jnp.clip(rank_ref[i : i + 1, :] - mine[:, i : i + 1], -1.0, 1.0)
            payoff_ref[i, at : at + step, :] = jnp.where(free, sign, 0.0).astype(PAYOFF)
    for copy in copies:
        copy.wait()
    section = lax.axis_index("section")
    pair, node = section // NODES, section % NODES
    lane = lax.broadcasted_iota(jnp.int32, (1, W), 1)
    for slot in range(SLOTS):
        alive_ref[slot : slot + 1, :] = jnp.broadcast_to(
            (live_ref[slot] > 0).astype(jnp.float32), (1, W)
        )
    for i in range(PAIR):
        words = [jnp.int32(0), jnp.int32(0)]
        for c in range(5):
            card = board_ref[PAIR * pair + i, c]
            bit = lax.shift_left(jnp.int32(1), card & 31)
            words[0] |= jnp.where(card < 32, bit, 0)
            words[1] |= jnp.where(card < 32, 0, bit)
        free = (((low & words[0]) | (high & words[1])) == 0) & (lane < H)
        mask_ref[i : i + 1, :] = jnp.where(free, 1.0, 0.0)
        pair_ref[i : i + 1, :] = jnp.broadcast_to(
            (live_ref[PAIR * pair + i] > 0).astype(jnp.float32), (1, W)
        )
    mask = mask_ref[...]
    for p in range(2):
        reach_ref[p] = jnp.zeros((PAIR, W), jnp.float32)
        value_ref[p] = jnp.where(lane == H, 1.0, jnp.zeros((PAIR, W), jnp.float32))
        reach_ref[p, :, :H] = root_ref[p, pl.ds(node, 1), :] * mask[:, :H]
        value_ref[p, :, :H] = frontier_ref[p, pl.ds(node, 1), :] * mask[:, :H]


def play(
    go_ref, payoff_ref, reach_ref, value_ref, mask_ref, alive_ref, sum_ref, gap_ref, x_ref, leaf_ref
):
    reach = [reach_ref[p] for p in range(2)]
    for s in range(DEPTHS):
        q = s % 2
        go = go_ref[PLACE[s]]
        mine = reach[q] * (1.0 - go)
        for i in range(PAIR):
            x_ref[i, 2 * s + 1 - q, :] = mine[i]
            x_ref[i, 2 * s + q, :] = reach[1 - q][i]
        reach[q] = reach[q] * go
    for i in range(PAIR):
        leaf = jnp.dot(
            x_ref[i].astype(jnp.bfloat16),
            payoff_ref[i].astype(jnp.bfloat16),
            preferred_element_type=jnp.float32,
        )
        leaf_ref[:, i, :] = leaf * mask_ref[i : i + 1, :]
    value = [value_ref[p] for p in range(2)]
    alive = alive_ref[...]
    for s in reversed(range(DEPTHS)):
        q = s % 2
        go = go_ref[PLACE[s]]
        leaf_mine, leaf_other = leaf_ref[2 * s + q], leaf_ref[2 * s + 1 - q]
        gap_ref[PLACE[s]] = leaf_mine - value[q]
        value[q] = (1.0 - go) * leaf_mine + go * value[q]
        value[1 - q] = leaf_other + value[1 - q]
        for p in range(2):
            weighted = alive * value[p]
            sum_ref[SUM_PLACE[s], p : p + 1, :] = weighted[0:1] + weighted[1:2]


def add_pairs(part_ref, out_ref):
    for p in range(2):
        for node in range(NODES):
            pair = [part_ref[SUM_PLACE[i * NODES + node], p : p + 1, :] for i in range(2)]
            total = pair[0] + pair[1]
            out_ref[p * NODES + node : p * NODES + node + 1, :] = total


def conclude(
    own_ref, part_x, part_y, part_z, stop_ref, go_ref, back_ref, alive_ref,
    new_stop_hbm, new_go_hbm, value_hbm,
    new_stop_ref, new_go_ref, value_ref, gap_ref, sem,
):
    total = own_ref[...] + part_x[...] + part_y[...] + part_z[...]
    value = total[:, :H] / total[:, H : H + 1]
    for p in range(2):
        value_ref[p] = value[p * NODES : (p + 1) * NODES]
    copies = [pltpu.make_async_copy(value_ref, value_hbm, sem.at[SLOTS, 0])]
    copies[0].start()
    for slot in range(SLOTS):
        for node in range(NODES):
            gap_ref[slot, node, :] = back_ref[PLACE[slot // PAIR * NODES + node], slot % PAIR, :]
        stop, go = stop_ref[slot], go_ref[slot]
        total = stop + go
        gap = gap_ref[slot, :, :H]
        keep = alive_ref[slot : slot + 1, :H] > 0
        new_stop_ref[slot] = jnp.where(keep, jnp.maximum(stop + go / total * gap, 0.0), stop)
        new_go_ref[slot] = jnp.where(keep, jnp.maximum(go - stop / total * gap, 0.0), go)
        for k, (src, dst) in enumerate(((new_stop_ref, new_stop_hbm), (new_go_ref, new_go_hbm))):
            copy = pltpu.make_async_copy(src.at[slot], dst.at[slot], sem.at[slot, k])
            copy.start()
            copies.append(copy)
    for copy in copies:
        copy.wait()


def call(body, out, specs, scratch=(), flops=100_000, limit=24 << 20, out_spec=VMEM):
    many = isinstance(out, list)
    return pl.pallas_call(
        body,
        out_shape=out,
        in_specs=specs,
        out_specs=[out_spec] * len(out) if many else out_spec,
        scratch_shapes=list(scratch),
        compiler_params=pltpu.CompilerParams(vmem_limit_bytes=limit),
        cost_estimate=pl.CostEstimate(flops=flops, bytes_accessed=400_000, transcendentals=0),
        name=body.__name__,
    )


def in_hbm(value):
    return pltpu.with_memory_space_constraint(value, pltpu.HBM)


def f32(*shape):
    return jax.ShapeDtypeStruct(shape, jnp.float32)


def exchange(value, order=ORDER):
    return lax.all_to_all(value, "section", 0, 0, axis_index_groups=[order], tiled=True)


def from_others(value, axis):
    return [
        lax.ppermute(value, axis, [(k, k ^ d) for k in range(SIDE)]) for d in (3, 1, 2)
    ]


def local(root_reach, frontier_value, regret_stop, regret_go, board_live, board_cards, hand_rank):
    stop_now, go_now = regret_stop[0], regret_go[0]
    block = pltpu.VMEM((SLOTS, NODES, H), jnp.float32)
    sent, ranks, cards = call(
        pack_go,
        [
            pltpu.VMEM((DEPTHS, PAIR, W), jnp.float32),
            pltpu.VMEM((8, W), jnp.float32),
            pltpu.VMEM((2, W), jnp.int32),
        ],
        [HBM] * 4,
        [
            block,
            block,
            pltpu.VMEM((SLOTS, H), jnp.int32),
            pltpu.SemaphoreType.DMA((SLOTS + 1, 2)),
        ],
    )(*[in_hbm(a) for a in (stop_now, go_now, hand_rank, card_masks())])
    go_all = exchange(sent)
    payoff, reach, value, mask, alive, alive_pair = call(
        prepare,
        [
            jax.ShapeDtypeStruct((PAIR, W, W), PAYOFF),
            f32(2, PAIR, W),
            f32(2, PAIR, W),
            f32(PAIR, W),
            f32(SLOTS, W),
            f32(PAIR, W),
        ],
        [VMEM] * 2 + [HBM] * 4,
        [
            pltpu.VMEM((2, NODES, H), jnp.float32),
            pltpu.VMEM((2, NODES, H), jnp.float32),
            pltpu.SMEM((SLOTS, 5), jnp.int32),
            pltpu.SMEM((SLOTS,), jnp.int32),
            pltpu.SemaphoreType.DMA((4,)),
        ],
        flops=20_000_000,
    )(ranks, cards, *[in_hbm(a) for a in (root_reach, frontier_value, board_cards, board_live)])
    sums, gaps = call(
        play,
        [pltpu.VMEM((DEPTHS, 2, W), jnp.float32), pltpu.VMEM((DEPTHS, PAIR, W), jnp.float32)],
        [VMEM] * 6,
        [
            pltpu.VMEM((PAIR, 2 * DEPTHS, W), jnp.float32),
            pltpu.VMEM((2 * DEPTHS, PAIR, W), jnp.float32),
        ],
        flops=250_000_000,
    )(go_all, payoff, reach, value, mask, alive_pair)
    sums = exchange(sums, SUM_ORDER)
    gaps = exchange(gaps)
    total = call(add_pairs, f32(2 * NODES, W), [VMEM])(sums)
    total = sum(from_others(total, "y"), start=total)
    parts = from_others(total, "x")
    new_stop, new_go, section_value = call(
        conclude,
        [f32(SLOTS, NODES, H), f32(SLOTS, NODES, H), f32(2, NODES, H)],
        [VMEM] * 8,
        [
            block,
            block,
            pltpu.VMEM((2, NODES, H), jnp.float32),
            pltpu.VMEM((SLOTS, NODES, W), jnp.float32),
            pltpu.SemaphoreType.DMA((SLOTS + 1, 2)),
        ],
        flops=2_000_000,
        out_spec=HBM,
    )(total, *parts, stop_now, go_now, gaps, alive)
    return (new_stop[None], new_go[None], section_value[None])


def solution(mesh):
    finer = Mesh(mesh.devices.reshape(DEPTHS, SIDE, SIDE), ("section", "y", "x"))
    board = ("y", "x")
    return jax.shard_map(
        local,
        mesh=finer,
        in_specs=(
            P(),
            P(),
            P("section", board, None, None),
            P("section", board, None, None),
            P(board),
            P(board, None),
            P(board, None),
        ),
        out_specs=(
            P("section", board, None, None),
            P("section", board, None, None),
            P("section", None, None, None),
        ),
        check_vma=False,
    )
```

```python
import jax
import jax.numpy as jnp
import numpy as np
from jax import lax
from jax.experimental import pallas as pl
from jax.experimental.pallas import tpu as pltpu
from jax.sharding import Mesh
from jax.sharding import PartitionSpec as P

CARDS = 52
H = 1326
W = 1408
NODES = 8
SLOTS = 4
DEPTHS = 16
ORDER = [*range(15, -1, -2), *range(14, -1, -2)]
PLACE = [ORDER.index(s) for s in range(DEPTHS)]
SUM_ORDER = [*range(15, -1, -2), *range(0, 16, 2)]
SUM_PLACE = [SUM_ORDER.index(s) for s in range(DEPTHS)]
PAIR = 2
SIDE = 4
MOST = 60_000_000
PAYOFF = jnp.float4_e2m1fn

VMEM = pl.BlockSpec(memory_space=pltpu.VMEM)
HBM = pl.BlockSpec(memory_space=pltpu.HBM)


def card_masks():
    hands = np.zeros((2, W), np.uint32)
    for cards in np.triu_indices(CARDS, 1):
        for word in range(2):
            inside = cards // 32 == word
            hands[word, :H] |= np.where(inside, np.uint32(1) << (cards % 32).astype(np.uint32), 0).astype(np.uint32)
    return jnp.asarray(hands.view(np.int32))


def pack_go(stop_hbm, go_hbm, rank_hbm, card_hbm, out_ref, rank_out, card_out, stop_ref, go_ref, rank_ref, sem):
    copies = []
    for slot in range(SLOTS):
        for k, (src, dst) in enumerate(((stop_hbm, stop_ref), (go_hbm, go_ref))):
            copy = pltpu.make_async_copy(src.at[slot], dst.at[slot], sem.at[slot, k])
            copy.start()
            copies.append(copy)
    rank_copy = pltpu.make_async_copy(rank_hbm, rank_ref, sem.at[SLOTS, 0])
    card_copy = pltpu.make_async_copy(card_hbm, card_out, sem.at[SLOTS, 1])
    rank_copy.start()
    card_copy.start()
    out_ref[:, :, 1280:] = jnp.ones((DEPTHS, PAIR, W - 1280), jnp.float32)
    rank_out[...] = jnp.zeros((8, W), jnp.float32)
    for slot in range(SLOTS):
        copies[2 * slot].wait()
        copies[2 * slot + 1].wait()
        go = go_ref[slot]
        prob = go / (stop_ref[slot] + go)
        for node in range(NODES):
            out_ref[PLACE[slot // PAIR * NODES + node], slot % PAIR, :H] = prob[node]
    rank_copy.wait()
    pair = lax.axis_index("section") // NODES
    for i in range(PAIR):
        rank_out[i : i + 1, :H] = rank_ref[pl.ds(PAIR * pair + i, 1), :].astype(jnp.float32)
    card_copy.wait()


def prepare(
    rank_ref, card_ref, root_hbm, frontier_hbm, board_hbm, live_hbm,
    payoff_ref, reach_ref, value_ref, mask_ref, alive_ref, pair_ref,
    root_ref, frontier_ref, board_ref, live_ref, sem,
):
    copies = [
        pltpu.make_async_copy(src, dst, sem.at[k])
        for k, (src, dst) in enumerate(
            (
                (root_hbm, root_ref),
                (frontier_hbm, frontier_ref),
                (board_hbm, board_ref),
                (live_hbm, live_ref),
            )
        )
    ]
    for copy in copies:
        copy.start()
    low, high = card_ref[0:1, :], card_ref[1:2, :]
    rank_column = rank_ref[...].T
    card_column = jnp.concatenate([card_ref[...], jnp.zeros((6, W), jnp.int32)], axis=0).T
    step = 64
    for at in range(0, W, step):
        mine = rank_column[at : at + step]
        low_mine = card_column[at : at + step, 0:1]
        high_mine = card_column[at : at + step, 1:2]
        free = ((low_mine & low) | (high_mine & high)) == 0
        for i in range(PAIR):
            sign = jnp.clip(rank_ref[i : i + 1, :] - mine[:, i : i + 1], -1.0, 1.0)
            payoff_ref[i, at : at + step, :] = jnp.where(free, sign, 0.0).astype(PAYOFF)
    for copy in copies:
        copy.wait()
    section = lax.axis_index("section")
    pair, node = section // NODES, section % NODES
    lane = lax.broadcasted_iota(jnp.int32, (1, W), 1)
    for slot in range(SLOTS):
        alive_ref[slot : slot + 1, :] = jnp.broadcast_to(
            (live_ref[slot] > 0).astype(jnp.float32), (1, W)
        )
    for i in range(PAIR):
        words = [jnp.int32(0), jnp.int32(0)]
        for c in range(5):
            card = board_ref[PAIR * pair + i, c]
            bit = lax.shift_left(jnp.int32(1), card & 31)
            words[0] |= jnp.where(card < 32, bit, 0)
            words[1] |= jnp.where(card < 32, 0, bit)
        free = (((low & words[0]) | (high & words[1])) == 0) & (lane < H)
        mask_ref[i : i + 1, :] = jnp.where(free, 1.0, 0.0)
        pair_ref[i : i + 1, :] = jnp.broadcast_to(
            (live_ref[PAIR * pair + i] > 0).astype(jnp.float32), (1, W)
        )
    mask = mask_ref[...]
    for p in range(2):
        reach_ref[p] = jnp.zeros((PAIR, W), jnp.float32)
        value_ref[p] = jnp.where(lane == H, 1.0, jnp.zeros((PAIR, W), jnp.float32))
        reach_ref[p, :, :H] = root_ref[p, pl.ds(node, 1), :] * mask[:, :H]
        value_ref[p, :, :H] = frontier_ref[p, pl.ds(node, 1), :] * mask[:, :H]


def play(
    go_ref, payoff_ref, reach_ref, value_ref, mask_ref, alive_ref, sum_ref, gap_ref, x_ref, leaf_ref
):
    reach = [reach_ref[p] for p in range(2)]
    for s in range(DEPTHS):
        q = s % 2
        go = go_ref[PLACE[s]]
        mine = reach[q] * (1.0 - go)
        for i in range(PAIR):
            x_ref[i, 2 * s + 1 - q, :] = mine[i]
            x_ref[i, 2 * s + q, :] = reach[1 - q][i]
        reach[q] = reach[q] * go
    for i in range(PAIR):
        leaf = jnp.dot(
            x_ref[i].astype(jnp.bfloat16),
            payoff_ref[i].astype(jnp.bfloat16),
            preferred_element_type=jnp.float32,
        )
        leaf_ref[:, i, :] = leaf * mask_ref[i : i + 1, :]
    value = [value_ref[p] for p in range(2)]
    alive = alive_ref[...]
    for s in reversed(range(DEPTHS)):
        q = s % 2
        go = go_ref[PLACE[s]]
        leaf_mine, leaf_other = leaf_ref[2 * s + q], leaf_ref[2 * s + 1 - q]
        gap_ref[PLACE[s]] = leaf_mine - value[q]
        value[q] = (1.0 - go) * leaf_mine + go * value[q]
        value[1 - q] = leaf_other + value[1 - q]
        for p in range(2):
            weighted = alive * value[p]
            sum_ref[SUM_PLACE[s], p : p + 1, :] = weighted[0:1] + weighted[1:2]


def add_pairs(part_ref, out_ref):
    for p in range(2):
        for node in range(NODES):
            pair = [part_ref[SUM_PLACE[i * NODES + node], p : p + 1, :] for i in range(2)]
            total = pair[0] + pair[1]
            out_ref[p * NODES + node : p * NODES + node + 1, :] = total


def conclude(
    own_ref, part_x, part_y, part_z, stop_ref, go_ref, back_ref, alive_ref,
    new_stop_hbm, new_go_hbm, value_hbm,
    new_stop_ref, new_go_ref, value_ref, gap_ref, sem,
):
    total = own_ref[...] + part_x[...] + part_y[...] + part_z[...]
    value = total[:, :H] / total[:, H : H + 1]
    for p in range(2):
        value_ref[p] = value[p * NODES : (p + 1) * NODES]
    copies = [pltpu.make_async_copy(value_ref, value_hbm, sem.at[SLOTS, 0])]
    copies[0].start()
    for slot in range(SLOTS):
        for node in range(NODES):
            gap_ref[slot, node, :] = back_ref[PLACE[slot // PAIR * NODES + node], slot % PAIR, :]
        stop, go = stop_ref[slot], go_ref[slot]
        total = stop + go
        gap = gap_ref[slot, :, :H]
        keep = alive_ref[slot : slot + 1, :H] > 0
        new_stop_ref[slot] = jnp.where(keep, jnp.maximum(stop + go / total * gap, 0.0), stop)
        new_go_ref[slot] = jnp.where(keep, jnp.maximum(go - stop / total * gap, 0.0), go)
        for k, (src, dst) in enumerate(((new_stop_ref, new_stop_hbm), (new_go_ref, new_go_hbm))):
            copy = pltpu.make_async_copy(src.at[slot], dst.at[slot], sem.at[slot, k])
            copy.start()
            copies.append(copy)
    for copy in copies:
        copy.wait()


def call(body, out, specs, scratch=(), flops=100_000, limit=24 << 20, out_spec=VMEM):
    many = isinstance(out, list)
    return pl.pallas_call(
        body,
        out_shape=out,
        in_specs=specs,
        out_specs=[out_spec] * len(out) if many else out_spec,
        scratch_shapes=list(scratch),
        compiler_params=pltpu.CompilerParams(vmem_limit_bytes=limit),
        cost_estimate=pl.CostEstimate(flops=flops, bytes_accessed=400_000, transcendentals=0),
        name=body.__name__,
    )


def in_hbm(value):
    return pltpu.with_memory_space_constraint(value, pltpu.HBM)


def f32(*shape):
    return jax.ShapeDtypeStruct(shape, jnp.float32)


def exchange(value, order=ORDER):
    return lax.all_to_all(value, "section", 0, 0, axis_index_groups=[order], tiled=True)


def from_others(value, axis):
    return [
        lax.ppermute(value, axis, [(k, k ^ d) for k in range(SIDE)]) for d in (1, 3, 2)
    ]


def local(root_reach, frontier_value, regret_stop, regret_go, board_live, board_cards, hand_rank):
    stop_now, go_now = regret_stop[0], regret_go[0]
    block = pltpu.VMEM((SLOTS, NODES, H), jnp.float32)
    sent, ranks, cards = call(
        pack_go,
        [
            pltpu.VMEM((DEPTHS, PAIR, W), jnp.float32),
            pltpu.VMEM((8, W), jnp.float32),
            pltpu.VMEM((2, W), jnp.int32),
        ],
        [HBM] * 4,
        [
            block,
            block,
            pltpu.VMEM((SLOTS, H), jnp.int32),
            pltpu.SemaphoreType.DMA((SLOTS + 1, 2)),
        ],
    )(*[in_hbm(a) for a in (stop_now, go_now, hand_rank, card_masks())])
    go_all = exchange(sent)
    payoff, reach, value, mask, alive, alive_pair = call(
        prepare,
        [
            jax.ShapeDtypeStruct((PAIR, W, W), PAYOFF),
            f32(2, PAIR, W),
            f32(2, PAIR, W),
            f32(PAIR, W),
            f32(SLOTS, W),
            f32(PAIR, W),
        ],
        [VMEM] * 2 + [HBM] * 4,
        [
            pltpu.VMEM((2, NODES, H), jnp.float32),
            pltpu.VMEM((2, NODES, H), jnp.float32),
            pltpu.SMEM((SLOTS, 5), jnp.int32),
            pltpu.SMEM((SLOTS,), jnp.int32),
            pltpu.SemaphoreType.DMA((4,)),
        ],
        flops=20_000_000,
    )(ranks, cards, *[in_hbm(a) for a in (root_reach, frontier_value, board_cards, board_live)])
    sums, gaps = call(
        play,
        [pltpu.VMEM((DEPTHS, 2, W), jnp.float32), pltpu.VMEM((DEPTHS, PAIR, W), jnp.float32)],
        [VMEM] * 6,
        [
            pltpu.VMEM((PAIR, 2 * DEPTHS, W), jnp.float32),
            pltpu.VMEM((2 * DEPTHS, PAIR, W), jnp.float32),
        ],
        flops=250_000_000,
    )(go_all, payoff, reach, value, mask, alive_pair)
    sums = exchange(sums, SUM_ORDER)
    gaps = exchange(gaps)
    total = call(add_pairs, f32(2 * NODES, W), [VMEM])(sums)
    total = sum(from_others(total, "y"), start=total)
    parts = from_others(total, "x")
    new_stop, new_go, section_value = call(
        conclude,
        [f32(SLOTS, NODES, H), f32(SLOTS, NODES, H), f32(2, NODES, H)],
        [VMEM] * 8,
        [
            block,
            block,
            pltpu.VMEM((2, NODES, H), jnp.float32),
            pltpu.VMEM((SLOTS, NODES, W), jnp.float32),
            pltpu.SemaphoreType.DMA((SLOTS + 1, 2)),
        ],
        flops=2_000_000,
        out_spec=HBM,
    )(total, *parts, stop_now, go_now, gaps, alive)
    return (new_stop[None], new_go[None], section_value[None])


def solution(mesh):
    finer = Mesh(mesh.devices.reshape(DEPTHS, SIDE, SIDE), ("section", "y", "x"))
    board = ("y", "x")
    return jax.shard_map(
        local,
        mesh=finer,
        in_specs=(
            P(),
            P(),
            P("section", board, None, None),
            P("section", board, None, None),
            P(board),
            P(board, None),
            P(board, None),
        ),
        out_specs=(
            P("section", board, None, None),
            P("section", board, None, None),
            P("section", None, None, None),
        ),
        check_vma=False,
    )
```
